256 devices in a mesh: img: 4 (over x), seq: 8 (over z_lo, y), tp: 8 (over z_hi, core).
Axes of the slice: x: 4, y: 4, z: 8 (z_hi: 4, z_lo: 2; z = z_hi * 2 + z_lo), core: 2. Of those that a mesh axis runs over, the one named last changes fastest.
Arguments:
- vit_qkv: bfloat16 [4, 4096, 3, 1280], P('img', ('seq', 'tp')), may hold values from -6 to 6
- patch_counts: int32 [4], P('img'), may hold values from 1024 to 4096, as said below
- vit_out_weight: bfloat16 [1280, 1280], replicated, may hold values from -0.15625 to 0.15625
- vit_norm_gain: float32 [1280], replicated, may hold values from 0.25 to 1.75
- merger_weight: bfloat16 [5120, 8192], P(('img', 'seq'), 'tp'), may hold values from -8 to 8
- lm_norm_gain: float32 [8192], P('tp'), may hold values from 0.25 to 1.75
- kv_weight: bfloat16 [8192, 2048], P('tp', ('img', 'seq')), may hold values from -0.0625 to 0.0625
- queries: bfloat16 [4, 4096, 64, 128], P('img', 'seq', 'tp'), may hold values from -6 to 6
- span_kv: bfloat16 [4, 4096, 2, 8, 128], P('img', 'seq', None, 'tp'), may hold values from -6 to 6
Outputs:
- lm_attention: bfloat16 [4, 4096, 64, 128], P('img', 'seq', 'tp')
The draws below stay inside these ranges and needn't reach their ends.
Inputs may be any that keep to these rules, and one draw needn't show every extreme that they name: `patch_counts`: each count is a multiple of 4, at least 1024, and some image has exactly 4096.
All inputs are finite; a program needn't handle non-finite values.
Results may differ from the reference program's by a relative error of at most 0.04.
Values may be sent and summed in bfloat16 or wider, within the bound.
A program may use at most 128 MiB of HBM per device.

```python
import math
import jax
import jax.numpy as jnp
from jax import lax

VIT_D = 1280
VIT_HEADS = 16
VIT_HDIM = 80
D = 8192
HQ = 64
KVH = 8
HD = 128
SPAN = 512
IMAGES = 4
PATCHES = 4096
VIS = 1024
TOKS = 4096
N_SEQ = 8


def draw_patch_counts(key, part):
    count_key, pick_key = jax.random.split(jax.random.fold_in(key, 11))
    counts = jax.random.randint(count_key, (IMAGES,), PATCHES // 16, PATCHES // 4 + 1) * 4
    chosen = jax.random.randint(pick_key, (), 0, IMAGES)
    return jnp.where(jnp.arange(IMAGES) == chosen, PATCHES, counts).astype(jnp.int32)


def base_field(key, shape):
    return jnp.clip(jax.random.normal(key, shape, jnp.float32), -6.0, 6.0)


def score_levels():
    return (110.0, 190.0, 290.0)


def plant_plan(level_key, target, head_size):
    parts = jax.random.split(level_key, 3)
    sign_vector = jnp.where(jax.random.bernoulli(parts[0], 0.5, (head_size,)), 1.0, -1.0).astype(jnp.float32)
    score_gap = jax.random.uniform(parts[1], (), jnp.float32, 1.0, 3.0)
    strength = min(math.sqrt(target / math.sqrt(head_size)), 5.9)
    top_score = strength * strength * math.sqrt(head_size)
    second_strength = strength * (top_score - score_gap) / top_score
    return (sign_vector, strength, second_strength, parts[2])


def draw_vit_qkv(key, part):
    base_key, plant_key = jax.random.split(jax.random.fold_in(key, 31))
    values = base_field(base_key, (IMAGES, PATCHES, 3, VIT_D))
    usable = PATCHES // 4
    for image_index in range(IMAGES):
        for level_index, target in enumerate(score_levels()):
            level_key = jax.random.fold_in(plant_key, image_index * 8 + level_index)
            sign_vector, strength, second_strength, pick_key = plant_plan(level_key, target, VIT_HDIM)
            picks = jax.random.split(pick_key, 4)
            query_slot = jax.random.randint(picks[0], (), 0, usable).astype(jnp.int32)
            first_slot = jax.random.randint(picks[1], (), 0, usable).astype(jnp.int32)
            second_slot = ((first_slot + 1 + jax.random.randint(picks[2], (), 0, usable - 1)) % usable).astype(jnp.int32)
            head_start = (jax.random.randint(picks[3], (), 0, VIT_HEADS) * VIT_HDIM).astype(jnp.int32)
            image_id = jnp.int32(image_index)
            values = lax.dynamic_update_slice(values, (strength * sign_vector).reshape(1, 1, 1, VIT_HDIM), (image_id, query_slot, jnp.int32(0), head_start))
            values = lax.dynamic_update_slice(values, (strength * sign_vector).reshape(1, 1, 1, VIT_HDIM), (image_id, first_slot, jnp.int32(1), head_start))
            values = lax.dynamic_update_slice(values, (second_strength * sign_vector).reshape(1, 1, 1, VIT_HDIM), (image_id, second_slot, jnp.int32(1), head_start))
    return values.astype(jnp.bfloat16)


def draw_merger_weight(key, part):
    rows_total = 4 * VIT_D
    parts = jax.random.split(jax.random.fold_in(key, 53), 2)
    column_place = jnp.arange(D, dtype=jnp.float32) / D
    jitter = jnp.exp(jax.random.uniform(parts[1], (D,), jnp.float32, -0.69, 0.69))
    column_scale = jnp.power(10.0, column_place) * jitter
    values = jax.random.normal(parts[0], (rows_total, D), jnp.float32) * rows_total ** (-0.5) * column_scale[None, :]
    return jnp.clip(values, -8.0, 8.0).astype(jnp.bfloat16)


def lm_plants(key):
    plans = []
    for image_index in range(IMAGES):
        for level_index, target in enumerate(score_levels()):
            level_key = jax.random.fold_in(key, image_index * 8 + level_index)
            sign_vector, strength, second_strength, pick_key = plant_plan(level_key, target, HD)
            picks = jax.random.split(pick_key, 5)
            sample_index = jax.random.randint(picks[0], (), 0, TOKS // SPAN)
            position = jax.random.randint(picks[1], (), SPAN // 2, SPAN)
            first_place = jax.random.randint(picks[2], (), 0, position + 1)
            second_place = (first_place + 1 + jax.random.randint(picks[3], (), 0, position)) % (position + 1)
            head_index = jax.random.randint(picks[4], (), 0, HQ).astype(jnp.int32)
            start = sample_index * SPAN
            plans.append((image_index, (start + position).astype(jnp.int32), (start + first_place).astype(jnp.int32), (start + second_place).astype(jnp.int32), head_index, sign_vector, strength, second_strength))
    return plans


def draw_queries(key, part):
    values = base_field(jax.random.fold_in(key, 41), (IMAGES, TOKS, HQ, HD))
    for image_index, query_token, first_token, second_token, head_index, sign_vector, strength, second_strength in lm_plants(jax.random.fold_in(key, 61)):
        values = lax.dynamic_update_slice(values, (strength * sign_vector).reshape(1, 1, 1, HD), (jnp.int32(image_index), query_token, head_index, jnp.int32(0)))
    return values.astype(jnp.bfloat16)


def draw_span_kv(key, part):
    values = base_field(jax.random.fold_in(key, 43), (IMAGES, TOKS, 2, KVH, HD))
    for image_index, query_token, first_token, second_token, head_index, sign_vector, strength, second_strength in lm_plants(jax.random.fold_in(key, 61)):
        kv_head = (head_index // (HQ // KVH)).astype(jnp.int32)
        image_id = jnp.int32(image_index)
        values = lax.dynamic_update_slice(values, (strength * sign_vector).reshape(1, 1, 1, 1, HD), (image_id, first_token, jnp.int32(0), kv_head, jnp.int32(0)))
        values = lax.dynamic_update_slice(values, (second_strength * sign_vector).reshape(1, 1, 1, 1, HD), (image_id, second_token, jnp.int32(0), kv_head, jnp.int32(0)))
    return values.astype(jnp.bfloat16)


def levels(stream_key, shape, cuts, low, largest):
    factor_of, own = 1.0, jax.random.fold_in(stream_key, 6)
    for dim, blocks in cuts:
        heights = jnp.exp(jax.random.uniform(jax.random.fold_in(own, dim), (blocks,), jnp.float32, low / len(cuts), largest / len(cuts)))
        factor_of = factor_of * jnp.repeat(heights, shape[dim] // blocks).reshape([-1 if axis == dim else 1 for axis in range(len(shape))])
    return factor_of


def normal_values(own_key, extent, deviation, most, pieces=(), held_as=jnp.bfloat16):
    drawn = deviation * jax.random.normal(own_key, extent, jnp.float32)
    if pieces:
        drawn = drawn * levels(own_key, extent, pieces, -0.22, 0.18)
    return jnp.clip(drawn, -most, most).astype(held_as)


def setup_inputs(seed: int = 0) -> dict:
    key_of = jax.random.split(jax.random.key(seed), 10)
    return {
        "vit_qkv": draw_vit_qkv(jax.random.fold_in(key_of[9], 71), 0),
        "patch_counts": draw_patch_counts(jax.random.fold_in(key_of[9], 71), 0),
        "vit_out_weight": normal_values(key_of[2], (VIT_D, VIT_D), VIT_D ** -0.5, 0.15625),
        "vit_norm_gain": jnp.clip(1.0 + 0.15 * jax.random.normal(key_of[3], (VIT_D,), jnp.float32), 0.25, 1.75),
        "merger_weight": draw_merger_weight(jax.random.fold_in(key_of[9], 71), 0),
        "lm_norm_gain": jnp.clip(1.0 + 0.15 * jax.random.normal(key_of[5], (D,), jnp.float32), 0.25, 1.75),
        "kv_weight": normal_values(key_of[6], (D, 2 * KVH * HD), D ** -0.5, 0.0625, ((0, 8), (1, 32))),
        "queries": draw_queries(jax.random.fold_in(key_of[9], 71), 0),
        "span_kv": draw_span_kv(jax.random.fold_in(key_of[9], 71), 0),
    }


masked_score = -1e+30

def vit_image(qkv_rows, patch_total, out_weight, norm_gain):
    slots = qkv_rows.shape[0]
    query_rows = qkv_rows[:, 0].reshape(slots, VIT_HEADS, VIT_HDIM).astype(jnp.float32)
    key_rows = qkv_rows[:, 1].reshape(slots, VIT_HEADS, VIT_HDIM).astype(jnp.float32)
    value_rows = qkv_rows[:, 2].reshape(slots, VIT_HEADS, VIT_HDIM).astype(jnp.float32)
    usable = jnp.arange(slots, dtype=jnp.int32) < patch_total
    block_rows = math.gcd(slots, 512)
    scaling = VIT_HDIM ** (-0.5)

    def attend(query_block):
        scores = jnp.einsum('qhd,khd->hqk', query_block, key_rows) * scaling
        scores = jnp.where(usable[None, None, :], scores, masked_score)
        peak = lax.optimization_barrier(jnp.max(scores, axis=-1, keepdims=True))
        weights = jnp.where(usable[None, None, :], jnp.exp(scores - peak), 0.0)
        weight_sum = lax.optimization_barrier(jnp.sum(weights, axis=-1))
        blended = jnp.einsum('hqk,khd->hqd', weights.astype(jnp.bfloat16).astype(jnp.float32), value_rows)
        return jnp.transpose(blended / weight_sum[..., None], (1, 0, 2))
    attended = lax.map(attend, query_rows.reshape(slots // block_rows, block_rows, VIT_HEADS, VIT_HDIM))
    attended = attended.reshape(slots, VIT_D).astype(jnp.bfloat16)
    hidden = jnp.dot(attended, out_weight, preferred_element_type=jnp.float32)
    hidden = jnp.where(usable[:, None], hidden, 0.0)
    centred = hidden - lax.optimization_barrier(jnp.mean(hidden, axis=-1, keepdims=True))
    spread = lax.optimization_barrier(jnp.mean(centred * centred, axis=-1, keepdims=True))
    normed = (centred * lax.rsqrt(spread + 1e-06) * norm_gain).astype(jnp.bfloat16)
    return normed.reshape(slots // 4, 4 * VIT_D)

def lm_image(query_rows, span_rows, visual_kv, visual_total):
    groups = HQ // KVH
    scaling = HD ** (-0.5)
    vis_keys = visual_kv[:, 0].astype(jnp.float32)
    vis_values = visual_kv[:, 1].astype(jnp.float32)
    usable = jnp.arange(VIS, dtype=jnp.int32) < visual_total
    causal = jnp.arange(SPAN)[:, None] >= jnp.arange(SPAN)[None, :]

    def sample(inputs):
        sample_queries, sample_span = inputs
        grouped = sample_queries.reshape(SPAN, KVH, groups, HD).astype(jnp.float32)
        far_scores = jnp.einsum('ckgd,nkd->kgcn', grouped, vis_keys) * scaling
        far_scores = jnp.where(usable[None, None, None, :], far_scores, masked_score)
        near_keys = sample_span[:, 0].astype(jnp.float32)
        near_values = sample_span[:, 1].astype(jnp.float32)
        near_scores = jnp.einsum('ckgd,nkd->kgcn', grouped, near_keys) * scaling
        near_scores = jnp.where(causal[None, None], near_scores, masked_score)
        peak = jnp.maximum(lax.optimization_barrier(jnp.max(far_scores, axis=-1)), lax.optimization_barrier(jnp.max(near_scores, axis=-1)))
        far_weights = jnp.where(usable[None, None, None, :], jnp.exp(far_scores - peak[..., None]), 0.0)
        near_weights = jnp.where(causal[None, None], jnp.exp(near_scores - peak[..., None]), 0.0)
        weight_sum = lax.optimization_barrier(jnp.sum(far_weights, axis=-1)) + lax.optimization_barrier(jnp.sum(near_weights, axis=-1))
        blended = jnp.einsum('kgcn,nkd->kgcd', far_weights.astype(jnp.bfloat16).astype(jnp.float32), vis_values)
        blended = blended + jnp.einsum('kgcn,nkd->kgcd', near_weights.astype(jnp.bfloat16).astype(jnp.float32), near_values)
        result = jnp.transpose(blended / weight_sum[..., None], (2, 0, 1, 3))
        return result.reshape(SPAN, HQ, HD).astype(jnp.bfloat16)
    result = lax.map(sample, (query_rows.reshape(N_SEQ, SPAN, HQ, HD), span_rows.reshape(N_SEQ, SPAN, 2, KVH, HD)))
    return result.reshape(TOKS, HQ, HD)

def reference(vit_qkv, patch_counts, vit_out_weight, vit_norm_gain, merger_weight, lm_norm_gain, kv_weight, queries, span_kv):

    def per_image(inputs):
        qkv_rows, patch_total, query_rows, span_rows = inputs
        merged = vit_image(qkv_rows, patch_total, vit_out_weight, vit_norm_gain)
        embedded = jnp.dot(merged, merger_weight, preferred_element_type=jnp.float32).astype(jnp.bfloat16)
        embedded_wide = lax.optimization_barrier(embedded).astype(jnp.float32)
        square_mean = lax.optimization_barrier(jnp.mean(embedded_wide * embedded_wide, axis=-1, keepdims=True))
        lm_normed = (embedded_wide * lax.rsqrt(square_mean + 1e-06) * lm_norm_gain).astype(jnp.bfloat16)
        visual_kv = jnp.dot(lm_normed, kv_weight, preferred_element_type=jnp.float32).astype(jnp.bfloat16)
        visual_kv = visual_kv.reshape(VIS, 2, KVH, HD)
        return lm_image(query_rows, span_rows, visual_kv, patch_total // 4)
    return lax.map(per_image, (vit_qkv, patch_counts, queries, span_kv))
```

```python
import jax
import jax.numpy as jnp
from jax import lax
from jax.experimental import pallas as pl
from jax.experimental.pallas import tpu as pltpu
from jax.sharding import Mesh
from jax.sharding import PartitionSpec as P

VIT_D = 1280
VIT_HEADS = 16
VIT_HDIM = 80
D = 8192
HQ = 64
KVH = 8
HD = 128
SEQ = ("zl", "y")
TP = ("zh", "c")
IMG_SEQ = ("x", "zl", "y")
MASKED = -1e30
LOG2E = 1.4426950408889634
F32 = jnp.float32
BF16 = jnp.bfloat16

ONE_AT, MASK_AT, KEY_AT, QUERY_AT, PACKED = 80, 81, 82, 162, 256
RING_ORDER = (0, 1, 7, 2, 6, 3, 5, 4)


def remote(src, dst, send_sem, recv_sem, **device):
    return pltpu.make_async_remote_copy(
        src_ref=src,
        dst_ref=dst,
        send_sem=send_sem,
        recv_sem=recv_sem,
        device_id=device,
        device_id_type=pl.DeviceIdType.MESH,
    )


def mod(a, n):
    return lax.rem(a, n)


def meet(peers):
    barrier = pltpu.get_barrier_semaphore()
    for device in peers:
        pl.semaphore_signal(
            barrier, inc=1, device_id=device, device_id_type=pl.DeviceIdType.MESH
        )
    pl.semaphore_wait(barrier, len(peers))


def nt_dot(a, b):
    return lax.dot_general(a, b, (((1,), (1,)), ((), ())), preferred_element_type=F32)


def vit_kernel(
    packed, wo, gain, live, tok_out,
    kv, qp, acc, peak, back, att, wov, nf, slab, mid, tok,
    a_s, a_r, y1_s, y1_r, y2_s, y2_r, o_s, o_r, m_s, m_r, t_s, t_r, w_sem, out_sem,
):
    y, zh, zl, c = (lax.axis_index(a) for a in ("y", "zh", "zl", "c"))
    z = zh * 2 + zl
    me = z * 2 + c
    up, down, across = mod(y + 1, 4), mod(y + 3, 4), mod(y + 2, 4)

    def place(dz, dc):
        other = mod(z + dz, 8)
        return other, mod(c + dc, 2)

    def device_of(other_z, other_c):
        return {"zh": lax.div(other_z, 2), "zl": mod(other_z, 2), "c": other_c}

    order = [(dz, dc) for dz in RING_ORDER for dc in range(2)]
    peers = [device_of(*place(dz, dc)) for dz, dc in order if (dz, dc) != (0, 0)]
    peers += [{"y": up}, {"y": down}, {"y": across}]
    meet(peers)

    sends = []
    for dz in (4, 3, 5, 2, 6, 1, 7, 0):
        for dc in range(2):
            if (dz, dc) == (0, 0):
                continue
            oz, oc = place(dz, dc)
            k = dz * 2 + dc
            copy = remote(
                packed.at[oz * 2 + oc], kv.at[y, me], a_s.at[k], a_r.at[k], **device_of(oz, oc)
            )
            copy.start()
            sends.append(copy)
    weights = []
    for h in range(VIT_HEADS):
        copy = pltpu.make_async_copy(
            wo.at[pl.ds(h * VIT_HDIM, VIT_HDIM)], wov.at[h, pl.ds(0, VIT_HDIM)], w_sem.at[h]
        )
        copy.start()
        weights.append(copy)
    kv[y, me] = packed[me]
    for h in range(VIT_HEADS):
        wov[h, VIT_HDIM:, :] = jnp.zeros((HD - VIT_HDIM, VIT_D), BF16)

    for i, (dz, dc) in enumerate(order):
        k = dz * 2 + dc
        source = mod(z + 8 - dz, 8) * 2 + mod(c + dc, 2)
        if k == 0:
            block = packed.at[me]
        else:
            block = kv.at[y, source]
            remote(block, block, a_s.at[k], a_r.at[k], y=up).wait_recv()
        for way, target in ((0, up), (1, down)):
            copy = remote(block, kv.at[y, source], y1_s.at[way, i], y1_r.at[way, i], y=target)
            copy.start()
            sends.append(copy)

    row = lax.broadcasted_iota(jnp.int32, (PACKED, PACKED), 0)
    col = lax.broadcasted_iota(jnp.int32, (PACKED, PACKED), 1)
    moved = (col >= KEY_AT) & (col < QUERY_AT) & (row == col + (QUERY_AT - KEY_AT))
    pick = moved | ((col == MASK_AT) & (row == ONE_AT))
    pick = jnp.where(pick, 1.0, 0.0).astype(BF16)
    scale = VIT_HDIM**-0.5 * LOG2E

    def fold(tile, slot, first):
        rows = pl.ds(pl.multiple_of(tile * 256, 256), 256)
        block = kv[slot].reshape(1024, PACKED)
        scores = nt_dot(qp[rows, :], block)
        top = jnp.max(scores, axis=1, keepdims=True)
        if first:
            weights = jnp.exp2((scores - top) * scale)
            total = jnp.dot(weights.astype(BF16), block, preferred_element_type=F32)
        else:
            old = peak[rows, :][:, :1]
            top = jnp.maximum(old, top)
            weights = jnp.exp2((scores - top) * scale)
            total = jnp.dot(weights.astype(BF16), block, preferred_element_type=F32)
            total += acc[rows, :] * jnp.exp2((old - top) * scale)
        peak[rows, :] = jnp.broadcast_to(top, (256, HD))
        return rows, total

    def whole(slot, first):
        def step(tile, carry):
            rows, total = fold(tile, slot, first)
            acc[rows, :] = total
            return carry

        lax.fori_loop(0, 4, step, 0)

    qp[...] = jnp.dot(
        kv[y].reshape(1024, PACKED), pick, preferred_element_type=F32
    ).astype(BF16)
    whole(y, True)

    for i, (dz, dc) in enumerate(order):
        source = mod(z + 8 - dz, 8) * 2 + mod(c + dc, 2)
        way, origin, target = ((0, down, up), (1, up, down))[i % 2]
        block = kv.at[origin, source]
        remote(block, block, y1_s.at[way, i], y1_r.at[way, i], y=up).wait_recv()
        copy = remote(block, block, y2_s.at[i], y2_r.at[i], y=target)
        copy.start()
        sends.append(copy)
    for i, (dz, dc) in enumerate(order):
        source = mod(z + 8 - dz, 8) * 2 + mod(c + dc, 2)
        way, origin = ((1, up), (0, down))[i % 2]
        block = kv.at[origin, source]
        remote(block, block, y1_s.at[way, i], y1_r.at[way, i], y=up).wait_recv()
    whole(down, False)
    whole(up, False)
    for i, (dz, dc) in enumerate(order):
        source = mod(z + 8 - dz, 8) * 2 + mod(c + dc, 2)
        block = kv.at[across, source]
        remote(block, block, y2_s.at[i], y2_r.at[i], y=up).wait_recv()

    def last(t, carry):
        tile = mod(zh + 1 + t, 4)
        _, total = fold(tile, across, False)
        done = (total[:, :HD] / total[:, ONE_AT : ONE_AT + 1]).astype(BF16)
        back[pl.ds(tile * 4, 4)] = done.reshape(4, 64, HD)
        for dzl in range(2):
            for dc in range(2):
                ozl, oc = mod(zl + dzl, 2), mod(c + dc, 2)
                k = t * 4 + dzl * 2 + dc
                copy = remote(
                    back.at[tile * 4 + ozl * 2 + oc], att.at[me], o_s.at[k], o_r.at[k],
                    zh=tile, zl=ozl, c=oc,
                )
                if dzl == 0 and dc == 0:
                    pl.when(t < 3)(copy.start)
                else:
                    copy.start()
        return carry

    lax.fori_loop(0, 4, last, 0)
    att[me] = back[me]
    for copy in weights:
        copy.wait()
    for t in range(4):
        for dzl in range(2):
            for dc in range(2):
                if (t, dzl, dc) == (3, 0, 0):
                    continue
                source = mod(zh + 3 - t, 4) * 4 + mod(zl + dzl, 2) * 2 + mod(c + dc, 2)
                k = t * 4 + dzl * 2 + dc
                copy = remote(att.at[source], att.at[source], o_s.at[k], o_r.at[k], y=up)
                copy.wait_recv()
                copy.wait_send()

    hidden = jnp.zeros((64, VIT_D), F32)
    for h in range(0, VIT_HEADS, 2):
        both = jnp.concatenate([att[h], att[h + 1]], axis=1)
        hidden += jnp.dot(
            both, wov[pl.ds(h, 2)].reshape(2 * HD, VIT_D), preferred_element_type=F32
        )
    hidden = jnp.where(live[...] > 0.0, hidden, 0.0)
    centred = hidden - jnp.mean(hidden, axis=1, keepdims=True)
    spread = jnp.mean(centred * centred, axis=1, keepdims=True)
    normed = (centred * lax.rsqrt(spread + 1e-6) * gain[...]).astype(BF16).astype(F32)
    for i in range(VIT_D // HD):
        nf[pl.ds(i * 64, 64), :] = normed[:, i * HD : (i + 1) * HD]

    lane = lax.broadcasted_iota(jnp.int32, (16, VIT_D), 1)
    quarter = [
        jnp.concatenate(
            [nf[pl.ds(i * 64 + j, 16, stride=4), :] for i in range(VIT_D // HD)], axis=1
        )
        for j in range(4)
    ]
    for part in range(4):
        out = jnp.zeros((16, VIT_D), F32)
        for j in range(4):
            for half in range(2):
                start = 320 * j + 160 * half
                origin = 640 * half + 160 * part
                shift = (start - origin) % VIT_D
                rolled = pltpu.roll(quarter[j], shift, 1) if shift else quarter[j]
                out = jnp.where((lane >= start) & (lane < start + 160), rolled, out)
        slab[part] = out.astype(BF16)
    for dy in range(1, 4):
        oy = mod(y + dy, 4)
        copy = remote(slab.at[oy], mid.at[y], m_s.at[dy], m_r.at[dy], y=oy)
        copy.start()
        sends.append(copy)
    mid[y] = slab[y]
    for dy in range(1, 4):
        source = mod(y + 4 - dy, 4)
        remote(mid.at[source], mid.at[source], m_s.at[dy], m_r.at[dy], y=up).wait_recv()

    right, left, far = mod(zh + 1, 4), mod(zh + 3, 4), mod(zh + 2, 4)
    oc = 1 - c
    mine = zh * 2 + c

    def pass_on(src, dst, k, **device):
        copy = remote(src, dst, t_s.at[k], t_r.at[k], **device)
        copy.start()
        sends.append(copy)

    def arrived(ref, k):
        remote(ref, ref, t_s.at[k], t_r.at[k], y=up).wait_recv()

    pass_on(mid, tok.at[mine], 0, zh=right)
    pass_on(mid, tok.at[mine], 1, zh=left)
    pass_on(mid, tok.at[mine], 2, c=oc)
    tok[mine] = mid[...]
    here = tok.at[left * 2 + c]
    arrived(here, 0)
    pass_on(here.at[pl.ds(0, 2)], here.at[pl.ds(0, 2)], 3, zh=right)
    pass_on(here, here, 4, c=oc)
    here = tok.at[right * 2 + c]
    arrived(here, 1)
    pass_on(here.at[pl.ds(2, 2)], here.at[pl.ds(2, 2)], 5, zh=left)
    pass_on(here, here, 6, c=oc)
    first, second = (tok.at[far * 2 + c].at[pl.ds(i, 2)] for i in (0, 2))
    arrived(first, 3)
    pass_on(first, first, 7, c=oc)
    arrived(second, 5)
    pass_on(second, second, 8, c=oc)
    arrived(tok.at[zh * 2 + oc], 2)
    arrived(tok.at[left * 2 + oc], 4)
    arrived(tok.at[right * 2 + oc], 6)
    arrived(tok.at[far * 2 + oc].at[pl.ds(0, 2)], 7)
    arrived(tok.at[far * 2 + oc].at[pl.ds(2, 2)], 8)
    for copy in sends:
        copy.wait_send()
    result = pltpu.make_async_copy(tok, tok_out, out_sem)
    result.start()
    result.wait()


def vit_tokens(packed, wo, gain, live):
    dma = pltpu.SemaphoreType.DMA
    vmem = pl.BlockSpec(memory_space=pltpu.VMEM)
    return pl.pallas_call(
        vit_kernel,
        out_shape=jax.ShapeDtypeStruct((8, 4, 16, VIT_D), BF16),
        in_specs=[vmem, pl.BlockSpec(memory_space=pl.ANY), vmem, vmem],
        out_specs=pl.BlockSpec(memory_space=pl.ANY),
        scratch_shapes=[
            pltpu.VMEM((4, 16, 64, PACKED), BF16),
            pltpu.VMEM((1024, PACKED), BF16),
            pltpu.VMEM((1024, PACKED), F32),
            pltpu.VMEM((1024, HD), F32),
            pltpu.VMEM((16, 64, HD), BF16),
            pltpu.VMEM((16, 64, HD), BF16),
            pltpu.VMEM((16, HD, VIT_D), BF16),
            pltpu.VMEM((64 * VIT_D // HD, HD), F32),
            pltpu.VMEM((4, 16, VIT_D), BF16),
            pltpu.VMEM((4, 16, VIT_D), BF16),
            pltpu.VMEM((8, 4, 16, VIT_D), BF16),
            dma((16,)), dma((16,)), dma((2, 16)), dma((2, 16)), dma((16,)), dma((16,)),
            dma((16,)), dma((16,)), dma((4,)), dma((4,)), dma((9,)), dma((9,)), dma((16,)), dma,
        ],
        compiler_params=pltpu.CompilerParams(collective_id=0, has_side_effects=True, vmem_limit_bytes=40 * 2**20),
        cost_estimate=pl.CostEstimate(flops=60_000_000_000, bytes_accessed=8_000_000, transcendentals=4_200_000),
        name="vit",
    )(packed, wo, gain, live)


def merge_kernel(
    tok, merger, kvw, gain, vis_out,
    mw, kw, sb, ra, rb, kvf, cs, cr, ks, ka, kb, ssr, vis,
    s_y, r_y, s_c, r_c, s_q, r_q, s_z, r_z, s_v, r_v, l_sem,
):
    y, zh, zl, c = (lax.axis_index(a) for a in ("y", "zh", "zl", "c"))
    up, down, across = mod(y + 1, 4), mod(y + 3, 4), mod(y + 2, 4)
    right, left, far = mod(zh + 1, 4), mod(zh + 3, 4), mod(zh + 2, 4)
    oc, ozl = 1 - c, 1 - zl
    load_m = pltpu.make_async_copy(merger, mw, l_sem.at[0])
    load_k = pltpu.make_async_copy(kvw, kw, l_sem.at[1])
    load_m.start()
    load_k.start()
    peers = [{"y": up}, {"y": down}, {"zl": ozl}]
    others = [(dzh, dc) for dzh in range(4) for dc in range(2) if dzh or dc]
    peers += [{"zh": mod(zh + dzh, 4), "c": mod(c + dc, 2)} for dzh, dc in others]
    meet(peers)
    sends = []

    def go(src, dst, ss, rs, **device):
        copy = remote(src, dst, ss, rs, **device)
        copy.start()
        sends.append(copy)

    def arrived(ref, ss, rs):
        remote(ref, ref, ss, rs, y=up).wait_recv()

    load_m.wait()

    def part(index):
        rows = pl.ds(pl.multiple_of(index * 128, 128), 128)
        return jnp.dot(tok[rows, :], mw[...], preferred_element_type=F32)

    sb[0] = part(across).astype(BF16)
    go(sb.at[0, pl.ds(0, 64)], ra.at[0], s_y.at[0], r_y.at[0], y=up)
    go(sb.at[0, pl.ds(64, 64)], ra.at[1], s_y.at[1], r_y.at[1], y=down)
    nxt, prv = part(up), part(down)
    arrived(ra.at[0], s_y.at[0], r_y.at[0])
    sb[1, 0:64] = (nxt[0:64] + ra[0].astype(F32)).astype(BF16)
    sb[1, 64:128] = nxt[64:128].astype(BF16)
    go(sb.at[1], rb.at[0], s_y.at[2], r_y.at[2], y=up)
    arrived(ra.at[1], s_y.at[1], r_y.at[1])
    sb[2, 0:64] = prv[0:64].astype(BF16)
    sb[2, 64:128] = (prv[64:128] + ra[1].astype(F32)).astype(BF16)
    go(sb.at[2], rb.at[1], s_y.at[3], r_y.at[3], y=down)
    own = part(y)
    arrived(rb.at[0], s_y.at[2], r_y.at[2])
    arrived(rb.at[1], s_y.at[3], r_y.at[3])
    embedded = (own + rb[0].astype(F32) + rb[1].astype(F32)).astype(BF16).astype(F32)
    square = jnp.sum(embedded * embedded, axis=1, keepdims=True)
    turned = jnp.transpose(jnp.broadcast_to(square, (128, 128)))
    ssr[zh * 2 + c] = turned[0:8]
    for k, (dzh, dc) in enumerate(others):
        slot = ssr.at[zh * 2 + c]
        go(slot, slot, s_q.at[k], r_q.at[k], zh=mod(zh + dzh, 4), c=mod(c + dc, 2))
    scaled = (embedded * gain[...]).astype(BF16)
    load_k.wait()
    for i in range(8):
        both = nt_dot(scaled, kw[pl.ds(i * 256, 256), :])
        kvf[2 * i] = both[:, :128]
        kvf[2 * i + 1] = both[:, 128:]

    for j in range(4):
        for k in range(2):
            cs[j, k] = kvf[k * 8 + j * 2 + oc].astype(BF16)
    go(cs, cr, s_c, r_c, c=oc)
    arrived(cr, s_c, r_c)

    def term(j, k):
        return kvf[k * 8 + j * 2 + c] + cr[j, k].astype(F32)

    for k in range(2):
        ks[0, k] = term(far, k).astype(BF16)
    go(ks.at[0, 0], ka.at[0], s_z.at[0], r_z.at[0], zh=right)
    go(ks.at[0, 1], ka.at[1], s_z.at[1], r_z.at[1], zh=left)
    arrived(ka.at[0], s_z.at[0], r_z.at[0])
    ks[1, 0] = (term(right, 0) + ka[0].astype(F32)).astype(BF16)
    ks[1, 1] = term(right, 1).astype(BF16)
    go(ks.at[1], kb.at[0], s_z.at[2], r_z.at[2], zh=right)
    arrived(ka.at[1], s_z.at[1], r_z.at[1])
    ks[2, 0] = term(left, 0).astype(BF16)
    ks[2, 1] = (term(left, 1) + ka[1].astype(F32)).astype(BF16)
    go(ks.at[2], kb.at[1], s_z.at[3], r_z.at[3], zh=left)
    for k, (dzh, dc) in enumerate(others):
        slot = ssr.at[mod(zh + 4 - dzh, 4) * 2 + mod(c + dc, 2)]
        arrived(slot, s_q.at[k], r_q.at[k])
    total = jnp.sum(ssr[...], axis=0)[0:1]
    factor = lax.rsqrt(jnp.broadcast_to(total, (128, 128)) / D + 1e-6)
    factor = jnp.transpose(factor)
    arrived(kb.at[0], s_z.at[2], r_z.at[2])
    arrived(kb.at[1], s_z.at[3], r_z.at[3])
    for k in range(2):
        done = term(zh, k) + kb[0, k].astype(F32) + kb[1, k].astype(F32)
        vis[y, zl, k] = (done * factor).astype(BF16)

    first = vis.at[y, zl]
    go(first, first, s_v.at[0], r_v.at[0], zl=ozl)
    go(first, first, s_v.at[1], r_v.at[1], y=up)
    go(first, first, s_v.at[2], r_v.at[2], y=down)
    second = vis.at[y, ozl]
    arrived(second, s_v.at[0], r_v.at[0])
    go(second, second, s_v.at[3], r_v.at[3], y=up)
    go(second, second, s_v.at[4], r_v.at[4], y=down)
    below = vis.at[down, zl]
    arrived(below, s_v.at[1], r_v.at[1])
    go(below, below, s_v.at[5], r_v.at[5], y=up)
    above = vis.at[up, ozl]
    arrived(above, s_v.at[4], r_v.at[4])
    go(above, above, s_v.at[6], r_v.at[6], y=down)
    arrived(vis.at[up, zl], s_v.at[2], r_v.at[2])
    arrived(vis.at[down, ozl], s_v.at[3], r_v.at[3])
    arrived(vis.at[across, zl], s_v.at[5], r_v.at[5])
    arrived(vis.at[across, ozl], s_v.at[6], r_v.at[6])
    for copy in sends:
        copy.wait_send()
    result = pltpu.make_async_copy(vis, vis_out, l_sem.at[2])
    result.start()
    result.wait()


def visual_keys_values(tok, merger, kvw, gain):
    dma = pltpu.SemaphoreType.DMA
    vmem = pl.BlockSpec(memory_space=pltpu.VMEM)
    hbm = pl.BlockSpec(memory_space=pl.ANY)
    return pl.pallas_call(
        merge_kernel,
        out_shape=jax.ShapeDtypeStruct((4, 2, 2, 128, 128), BF16),
        in_specs=[vmem, hbm, hbm, vmem],
        out_specs=hbm,
        scratch_shapes=[
            pltpu.VMEM((1280, 1024), BF16),
            pltpu.VMEM((2048, 1024), BF16),
            pltpu.VMEM((3, 128, 1024), BF16),
            pltpu.VMEM((2, 64, 1024), BF16),
            pltpu.VMEM((2, 128, 1024), BF16),
            pltpu.VMEM((16, 128, 128), F32),
            pltpu.VMEM((4, 2, 128, 128), BF16),
            pltpu.VMEM((4, 2, 128, 128), BF16),
            pltpu.VMEM((3, 2, 128, 128), BF16),
            pltpu.VMEM((2, 128, 128), BF16),
            pltpu.VMEM((2, 2, 128, 128), BF16),
            pltpu.VMEM((8, 8, 128), F32),
            pltpu.VMEM((4, 2, 2, 128, 128), BF16),
            dma((4,)), dma((4,)), dma, dma, dma((7,)), dma((7,)), dma((4,)), dma((4,)),
            dma((7,)), dma((7,)), dma((3,)),
        ],
        compiler_params=pltpu.CompilerParams(collective_id=1, has_side_effects=True, vmem_limit_bytes=40 * 2**20),
        cost_estimate=pl.CostEstimate(flops=20_000_000_000, bytes_accessed=8_000_000, transcendentals=0),
        name="merge",
    )(tok, merger, kvw, gain)


ROWS = 256


def lm_kernel(q, vis, span, bias, out):
    tile = pl.program_id(0)
    scale = HD**-0.5 * LOG2E
    ones = jnp.ones((1536, HD), BF16)
    keys = vis[:, :, 0].reshape(1024, HD)
    values = vis[:, :, 1].reshape(1024, HD)
    query = q[...]
    far = nt_dot(query, keys) + bias[...]
    near = nt_dot(query, span[0])
    token = (tile * ROWS + lax.broadcasted_iota(jnp.int32, (ROWS, 512), 0)) // 8
    place = lax.broadcasted_iota(jnp.int32, (ROWS, 512), 1)
    near = jnp.where(place <= token, near, MASKED)
    top = jnp.maximum(jnp.max(far, axis=1, keepdims=True), jnp.max(near, axis=1, keepdims=True))
    far = jnp.exp2((far - top) * scale).astype(BF16)
    near = jnp.exp2((near - top) * scale).astype(BF16)
    total = jnp.dot(
        far, jnp.concatenate([values, ones[:1024]], axis=1), preferred_element_type=F32
    ) + jnp.dot(near, jnp.concatenate([span[1], ones[:512]], axis=1), preferred_element_type=F32)
    out[...] = (total[:, :HD] / total[:, HD : HD + 1]).astype(BF16)


def lm_attention(q, vis, span, bias):
    whole = lambda *shape: pl.BlockSpec(shape, lambda i: (0,) * len(shape))
    rows = q.shape[0]
    return pl.pallas_call(
        lm_kernel,
        out_shape=jax.ShapeDtypeStruct((rows, HD), BF16),
        grid=(rows // ROWS,),
        in_specs=[
            pl.BlockSpec((ROWS, HD), lambda i: (i, 0)),
            whole(4, 2, 2, 128, 128),
            whole(2, 512, HD),
            whole(1, 1024),
        ],
        out_specs=pl.BlockSpec((ROWS, HD), lambda i: (i, 0)),
        compiler_params=pltpu.CompilerParams(vmem_limit_bytes=40 * 2**20),
        name="lm",
    )(q, vis, span, bias)


def pack_patches(vit_qkv, patch_total, first_patch):
    rows = vit_qkv.shape[1]
    split = vit_qkv[0].reshape(rows, 3, VIT_HEADS, VIT_HDIM).transpose(1, 2, 0, 3)
    ids = first_patch + jnp.arange(rows, dtype=jnp.int32)
    live = ids < patch_total
    mask = jnp.broadcast_to(
        jnp.where(live, 0.0, MASKED).astype(BF16)[None, :, None], (VIT_HEADS, rows, 1)
    )
    one = jnp.ones((VIT_HEADS, rows, 1), BF16)
    rest = jnp.zeros((VIT_HEADS, rows, PACKED - QUERY_AT - VIT_HDIM), BF16)
    packed = jnp.concatenate([split[2], one, mask, split[1], split[0], rest], axis=-1)
    return packed, live.astype(F32)[:, None]


def local(
    vit_qkv,
    patch_counts,
    vit_out_weight,
    vit_norm_gain,
    merger_weight,
    lm_norm_gain,
    kv_weight,
    queries,
    span_kv,
):
    patch_total = patch_counts[0]
    seq = lax.axis_index(SEQ)
    tp = lax.axis_index(TP)
    merger = lax.all_gather(merger_weight, ("x", "zl"), axis=0, tiled=True)
    kvw = lax.all_gather(kv_weight.T, IMG_SEQ, axis=0, tiled=True)
    packed, live = pack_patches(vit_qkv, patch_total, (seq * 8 + tp) * vit_qkv.shape[1])
    tok = vit_tokens(packed, vit_out_weight, vit_norm_gain[None], live)
    vis = visual_keys_values(tok.reshape(512, VIT_D), merger, kvw, lm_norm_gain[None])
    key = jnp.arange(1024, dtype=jnp.int32)
    block, r = key // 128, key % 128
    token = (((block % 2) * 4 + r // 16 % 4) * 8 + (block // 2) * 2 + r // 64) * 16 + r % 16
    bias = jnp.where(token < patch_total // 4, 0.0, MASKED)[None].astype(F32)
    rows = queries.shape[1] * queries.shape[2]
    span = span_kv[0, :, :, 0].transpose(1, 0, 2)
    out = lm_attention(queries.reshape(rows, HD), vis, span, bias)
    return out.reshape(queries.shape)


def solution(mesh):
    fine = Mesh(mesh.devices.reshape(4, 2, 4, 4, 2), ("x", "zl", "y", "zh", "c"))
    placed = (
        P("x", (*SEQ, *TP), None, None),
        P("x"),
        P(),
        P(),
        P(IMG_SEQ, TP),
        P(TP),
        P(TP, IMG_SEQ),
        P("x", SEQ, TP, None),
        P("x", SEQ, None, TP, None),
    )
    return jax.shard_map(
        local, mesh=fine, in_specs=placed, out_specs=P("x", SEQ, TP, None), check_vma=False
    )
```

```python
import jax
import jax.numpy as jnp
from jax import lax
from jax.experimental import pallas as pl
from jax.experimental.pallas import tpu as pltpu
from jax.sharding import Mesh
from jax.sharding import PartitionSpec as P

VIT_D = 1280
VIT_HEADS = 16
VIT_HDIM = 80
D = 8192
HQ = 64
KVH = 8
HD = 128
SEQ = ("zl", "y")
TP = ("zh", "c")
IMG_SEQ = ("x", "zl", "y")
MASKED = -1e30
LOG2E = 1.4426950408889634
F32 = jnp.float32
BF16 = jnp.bfloat16

ONE_AT, MASK_AT, KEY_AT, QUERY_AT, PACKED = 80, 81, 82, 162, 256
RING_ORDER = (0, 1, 7, 2, 6, 3, 5, 4)


def remote(src, dst, send_sem, recv_sem, **device):
    return pltpu.make_async_remote_copy(
        src_ref=src,
        dst_ref=dst,
        send_sem=send_sem,
        recv_sem=recv_sem,
        device_id=device,
        device_id_type=pl.DeviceIdType.MESH,
    )


def mod(a, n):
    return lax.rem(a, n)


def meet(peers):
    barrier = pltpu.get_barrier_semaphore()
    for device in peers:
        pl.semaphore_signal(
            barrier, inc=1, device_id=device, device_id_type=pl.DeviceIdType.MESH
        )
    pl.semaphore_wait(barrier, len(peers))


def nt_dot(a, b):
    return lax.dot_general(a, b, (((1,), (1,)), ((), ())), preferred_element_type=F32)


def front_kernel(
    packed, wo, gain, live, merger, kvw, lm_gain, vis_out,
    kv, qp, acc, peak, back, att, wov, nf, slab, mid, tok,
    mw, kw0, kw1, sb, ra, rb, kvf, cs, cr, ks, ka, kb, ssr, vis,
    o_s, o_r, w_sem, sent, got,
):
    x, y, zh, zl, c = (lax.axis_index(a) for a in ("x", "y", "zh", "zl", "c"))
    z = zh * 2 + zl
    me = z * 2 + c
    up, down, across = mod(y + 1, 4), mod(y + 3, 4), mod(y + 2, 4)
    right, left, far = mod(zh + 1, 4), mod(zh + 3, 4), mod(zh + 2, 4)
    east, west, xfar = mod(x + 1, 4), mod(x + 3, 4), mod(x + 2, 4)
    oc, ozl = 1 - c, 1 - zl

    def place(dz, dc):
        other = mod(z + dz, 8)
        return other, mod(c + dc, 2)

    def device_of(other_z, other_c):
        return {"zh": lax.div(other_z, 2), "zl": mod(other_z, 2), "c": other_c}

    order = [(dz, dc) for dz in RING_ORDER for dc in range(2)]
    peers = [device_of(*place(dz, dc)) for dz, dc in order if (dz, dc) != (0, 0)]
    peers += [{"y": up}, {"y": down}, {"y": across}, {"x": east}, {"x": west}]
    meet(peers)

    numbers, sends = {}, []

    def number(name):
        return numbers.setdefault(name, len(numbers))

    def go(name, src, dst, **device):
        k = number(name)
        copy = remote(src, dst, sent.at[k], got.at[k], **device)
        copy.start()
        sends.append(copy)

    def arrived(name, ref):
        k = number(name)
        remote(ref, ref, sent.at[k], got.at[k], y=up).wait_recv()

    for dz in (4, 3, 5, 2, 6, 1, 7, 0):
        for dc in range(2):
            if (dz, dc) != (0, 0):
                oz, oc_ = place(dz, dc)
                go(("a", dz, dc), packed.at[oz * 2 + oc_], kv.at[y, me], **device_of(oz, oc_))
    weights = []
    for h in range(VIT_HEADS):
        copy = pltpu.make_async_copy(
            wo.at[pl.ds(h * VIT_HDIM, VIT_HDIM)], wov.at[h, pl.ds(0, VIT_HDIM)], w_sem.at[h]
        )
        copy.start()
        weights.append(copy)

    low, high = pl.ds(0, 32), pl.ds(32, 32)
    go(("w", "e", 0), merger, mw.at[x, zl], x=east)
    go(("w", "w", 0), merger, mw.at[x, zl], x=west)
    go(("w", "z"), merger, mw.at[x, zl], zl=ozl)
    go(("k0", "z"), kvw.at[low], kw0.at[y, x, zl], zl=ozl)
    go(("k1", "z"), kvw.at[high], kw1.at[x, y, zl], zl=ozl)
    go(("k0", "e", 0), kvw.at[low], kw0.at[y, x, zl], x=east)
    go(("k0", "w", 0), kvw.at[low], kw0.at[y, x, zl], x=west)
    kv[y, me] = packed[me]
    mw[x, zl] = merger[...]
    kw0[y, x, zl] = kvw[0:32]
    kw1[x, y, zl] = kvw[32:64]
    for h in range(VIT_HEADS):
        wov[h, VIT_HDIM:, :] = jnp.zeros((HD - VIT_HDIM, VIT_D), BF16)

    def source_of(dz, dc):
        return mod(z + 8 - dz, 8) * 2 + mod(c + dc, 2)

    for i, (dz, dc) in enumerate(order):
        source = source_of(dz, dc)
        if i == 0:
            block = packed.at[me]
        else:
            block = kv.at[y, source]
            arrived(("a", dz, dc), block)
        go(("y1", 0, i), block, kv.at[y, source], y=up)
        go(("y1", 1, i), block, kv.at[y, source], y=down)

    row = lax.broadcasted_iota(jnp.int32, (PACKED, PACKED), 0)
    col = lax.broadcasted_iota(jnp.int32, (PACKED, PACKED), 1)
    moved = (col >= KEY_AT) & (col < QUERY_AT) & (row == col + (QUERY_AT - KEY_AT))
    pick = moved | ((col == MASK_AT) & (row == ONE_AT))
    pick = jnp.where(pick, 1.0, 0.0).astype(BF16)
    scale = VIT_HDIM**-0.5 * LOG2E

    def fold(tile, slot, first):
        rows = pl.ds(pl.multiple_of(tile * 256, 256), 256)
        block = kv[slot].reshape(1024, PACKED)
        scores = nt_dot(qp[rows, :], block)
        top = jnp.max(scores, axis=1, keepdims=True)
        if first:
            weights = jnp.exp2((scores - top) * scale)
            total = jnp.dot(weights.astype(BF16), block, preferred_element_type=F32)
        else:
            old = peak[rows, :][:, :1]
            top = jnp.maximum(old, top)
            weights = jnp.exp2((scores - top) * scale)
            total = jnp.dot(weights.astype(BF16), block, preferred_element_type=F32)
            total += acc[rows, :] * jnp.exp2((old - top) * scale)
        peak[rows, :] = jnp.broadcast_to(top, (256, HD))
        return rows, total

    def whole(slot, first):
        def step(tile, carry):
            rows, total = fold(tile, slot, first)
            acc[rows, :] = total
            return carry

        lax.fori_loop(0, 4, step, 0)

    qp[...] = jnp.dot(
        kv[y].reshape(1024, PACKED), pick, preferred_element_type=F32
    ).astype(BF16)
    whole(y, True)

    arrived(("w", "z"), mw.at[x, ozl])
    go(("w", "e", 1), mw.at[x, ozl], mw.at[x, ozl], x=east)
    go(("w", "w", 1), mw.at[x, ozl], mw.at[x, ozl], x=west)
    arrived(("k0", "z"), kw0.at[y, x, ozl])
    go(("k0", "e", 1), kw0.at[y, x, ozl], kw0.at[y, x, ozl], x=east)
    go(("k0", "w", 1), kw0.at[y, x, ozl], kw0.at[y, x, ozl], x=west)

    for i, (dz, dc) in enumerate(order):
        way, origin, target = ((0, down, up), (1, up, down))[i % 2]
        block = kv.at[origin, source_of(dz, dc)]
        arrived(("y1", way, i), block)
        go(("y2", i), block, block, y=target)
    for i, (dz, dc) in enumerate(order):
        way, origin = ((1, up), (0, down))[i % 2]
        arrived(("y1", way, i), kv.at[origin, source_of(dz, dc)])

    arrived(("k1", "z"), kw1.at[x, y, ozl])
    go(("k1", "u", 0), kvw.at[high], kw1.at[x, y, zl], y=up)
    go(("k1", "d", 0), kvw.at[high], kw1.at[x, y, zl], y=down)
    go(("k1", "u", 1), kw1.at[x, y, ozl], kw1.at[x, y, ozl], y=up)
    go(("k1", "d", 1), kw1.at[x, y, ozl], kw1.at[x, y, ozl], y=down)
    whole(down, False)
    arrived(("w", "e", 0), mw.at[west, zl])
    go(("w", "e", 2), mw.at[west, zl], mw.at[west, zl], x=east)
    arrived(("k0", "e", 0), kw0.at[y, west, zl])
    go(("k0", "e", 2), kw0.at[y, west, zl], kw0.at[y, west, zl], x=east)
    whole(up, False)
    arrived(("w", "w", 1), mw.at[east, ozl])
    go(("w", "w", 2), mw.at[east, ozl], mw.at[east, ozl], x=west)
    arrived(("k0", "w", 1), kw0.at[y, east, ozl])
    go(("k0", "w", 2), kw0.at[y, east, ozl], kw0.at[y, east, ozl], x=west)
    for i, (dz, dc) in enumerate(order):
        arrived(("y2", i), kv.at[across, source_of(dz, dc)])

    def last(t, carry):
        tile = mod(zh + 1 + t, 4)
        _, total = fold(tile, across, False)
        done = (total[:, :HD] / total[:, ONE_AT : ONE_AT + 1]).astype(BF16)
        back[pl.ds(tile * 4, 4)] = done.reshape(4, 64, HD)
        for dzl in range(2):
            for dc in range(2):
                tzl, tc = mod(zl + dzl, 2), mod(c + dc, 2)
                k = t * 4 + dzl * 2 + dc
                copy = remote(
                    back.at[tile * 4 + tzl * 2 + tc], att.at[me], o_s.at[k], o_r.at[k],
                    zh=tile, zl=tzl, c=tc,
                )
                if dzl == 0 and dc == 0:
                    pl.when(t < 3)(copy.start)
                else:
                    copy.start()
        return carry

    lax.fori_loop(0, 4, last, 0)
    att[me] = back[me]

    arrived(("k1", "u", 0), kw1.at[x, down, zl])
    go(("k1", "u", 2), kw1.at[x, down, zl], kw1.at[x, down, zl], y=up)
    arrived(("k1", "d", 1), kw1.at[x, up, ozl])
    go(("k1", "d", 2), kw1.at[x, up, ozl], kw1.at[x, up, ozl], y=down)
    arrived(("k0", "w", 0), kw0.at[y, east, zl])
    arrived(("k0", "e", 1), kw0.at[y, west, ozl])
    arrived(("k0", "e", 2), kw0.at[y, xfar, zl])
    arrived(("k0", "w", 2), kw0.at[y, xfar, ozl])
    for copy in weights:
        copy.wait()
    for t in range(4):
        for dzl in range(2):
            for dc in range(2):
                if (t, dzl, dc) == (3, 0, 0):
                    continue
                source = mod(zh + 3 - t, 4) * 4 + mod(zl + dzl, 2) * 2 + mod(c + dc, 2)
                k = t * 4 + dzl * 2 + dc
                copy = remote(att.at[source], att.at[source], o_s.at[k], o_r.at[k], y=up)
                copy.wait_recv()
                copy.wait_send()
    go(("k0", "u"), kw0.at[y], kw0.at[y], y=up)
    go(("k0", "d"), kw0.at[y], kw0.at[y], y=down)

    hidden = jnp.zeros((64, VIT_D), F32)
    for h in range(0, VIT_HEADS, 2):
        both = jnp.concatenate([att[h], att[h + 1]], axis=1)
        hidden += jnp.dot(
            both, wov[pl.ds(h, 2)].reshape(2 * HD, VIT_D), preferred_element_type=F32
        )
    hidden = jnp.where(live[...] > 0.0, hidden, 0.0)
    centred = hidden - jnp.mean(hidden, axis=1, keepdims=True)
    spread = jnp.mean(centred * centred, axis=1, keepdims=True)
    normed = (centred * lax.rsqrt(spread + 1e-6) * gain[...]).astype(BF16).astype(F32)
    for i in range(VIT_D // HD):
        nf[pl.ds(i * 64, 64), :] = normed[:, i * HD : (i + 1) * HD]

    lane = lax.broadcasted_iota(jnp.int32, (16, VIT_D), 1)
    quarter = [
        jnp.concatenate(
            [nf[pl.ds(i * 64 + j, 16, stride=4), :] for i in range(VIT_D // HD)], axis=1
        )
        for j in range(4)
    ]
    for part in range(4):
        out = jnp.zeros((16, VIT_D), F32)
        for j in range(4):
            for half in range(2):
                start = 320 * j + 160 * half
                origin = 640 * half + 160 * part
                shift = (start - origin) % VIT_D
                rolled = pltpu.roll(quarter[j], shift, 1) if shift else quarter[j]
                out = jnp.where((lane >= start) & (lane < start + 160), rolled, out)
        slab[part] = out.astype(BF16)
    for dy in range(1, 4):
        oy = mod(y + dy, 4)
        go(("m", dy), slab.at[oy], mid.at[y], y=oy)
    mid[y] = slab[y]
    for dy in range(1, 4):
        arrived(("m", dy), mid.at[mod(y + 4 - dy, 4)])

    mine = zh * 2 + c
    go("t0", mid, tok.at[mine], zh=right)
    go("t1", mid, tok.at[mine], zh=left)
    go("t2", mid, tok.at[mine], c=oc)
    tok[mine] = mid[...]
    arrived(("k1", "d", 0), kw1.at[x, up, zl])
    arrived(("k1", "u", 1), kw1.at[x, down, ozl])
    arrived(("k1", "u", 2), kw1.at[x, across, zl])
    arrived(("k1", "d", 2), kw1.at[x, across, ozl])
    go(("k1", "e"), kw1.at[x], kw1.at[x], x=east)
    go(("k1", "w"), kw1.at[x], kw1.at[x], x=west)
    here = tok.at[left * 2 + c]
    arrived("t0", here)
    go("t3", here.at[pl.ds(0, 2)], here.at[pl.ds(0, 2)], zh=right)
    go("t4", here, here, c=oc)
    here = tok.at[right * 2 + c]
    arrived("t1", here)
    go("t5", here.at[pl.ds(2, 2)], here.at[pl.ds(2, 2)], zh=left)
    go("t6", here, here, c=oc)
    first, second = (tok.at[far * 2 + c].at[pl.ds(i, 2)] for i in (0, 2))
    arrived("t3", first)
    go("t7", first, first, c=oc)
    arrived("t5", second)
    go("t8", second, second, c=oc)
    arrived(("k0", "u"), kw0.at[down])
    go(("k0", "u", 2), kw0.at[down, pl.ds(0, 2)], kw0.at[down, pl.ds(0, 2)], y=up)
    arrived(("k0", "d"), kw0.at[up])
    go(("k0", "d", 2), kw0.at[up, pl.ds(2, 2)], kw0.at[up, pl.ds(2, 2)], y=down)
    arrived("t2", tok.at[zh * 2 + oc])
    arrived("t4", tok.at[left * 2 + oc])
    arrived("t6", tok.at[right * 2 + oc])
    arrived("t7", tok.at[far * 2 + oc].at[pl.ds(0, 2)])
    arrived("t8", tok.at[far * 2 + oc].at[pl.ds(2, 2)])
    arrived(("w", "w", 0), mw.at[east, zl])
    arrived(("w", "e", 1), mw.at[west, ozl])
    arrived(("w", "e", 2), mw.at[xfar, zl])
    arrived(("w", "w", 2), mw.at[xfar, ozl])

    def part(index):
        rows = tok[pl.ds(index * 2, 2)].reshape(128, VIT_D)
        return jnp.dot(rows, mw[...].reshape(VIT_D, 1024), preferred_element_type=F32)

    sb[0] = part(across).astype(BF16)
    go("s0", sb.at[0, pl.ds(0, 64)], ra.at[0], y=up)
    go("s1", sb.at[0, pl.ds(64, 64)], ra.at[1], y=down)
    nxt, prv = part(up), part(down)
    arrived("s0", ra.at[0])
    sb[1, 0:64] = (nxt[0:64] + ra[0].astype(F32)).astype(BF16)
    sb[1, 64:128] = nxt[64:128].astype(BF16)
    go("s2", sb.at[1], rb.at[0], y=up)
    arrived("s1", ra.at[1])
    sb[2, 0:64] = prv[0:64].astype(BF16)
    sb[2, 64:128] = (prv[64:128] + ra[1].astype(F32)).astype(BF16)
    go("s3", sb.at[2], rb.at[1], y=down)
    own = part(y)
    arrived(("k1", "e"), kw1.at[west])
    go(("k1", "e", 2), kw1.at[west, pl.ds(0, 2)], kw1.at[west, pl.ds(0, 2)], x=east)
    arrived(("k1", "w"), kw1.at[east])
    go(("k1", "w", 2), kw1.at[east, pl.ds(2, 2)], kw1.at[east, pl.ds(2, 2)], x=west)
    arrived("s2", rb.at[0])
    arrived("s3", rb.at[1])
    embedded = (own + rb[0].astype(F32) + rb[1].astype(F32)).astype(BF16).astype(F32)
    square = jnp.sum(embedded * embedded, axis=1, keepdims=True)
    turned = jnp.transpose(jnp.broadcast_to(square, (128, 128)))
    others = [(dzh, dc) for dzh in range(4) for dc in range(2) if dzh or dc]
    ssr[zh * 2 + c] = turned[0:8]
    for dzh, dc in others:
        slot = ssr.at[zh * 2 + c]
        go(("q", dzh, dc), slot, slot, zh=mod(zh + dzh, 4), c=mod(c + dc, 2))
    scaled = (embedded * lm_gain[...]).astype(BF16)
    arrived(("k0", "u", 2), kw0.at[across, pl.ds(0, 2)])
    arrived(("k0", "d", 2), kw0.at[across, pl.ds(2, 2)])
    arrived(("k1", "e", 2), kw1.at[xfar, pl.ds(0, 2)])
    arrived(("k1", "w", 2), kw1.at[xfar, pl.ds(2, 2)])

    def head_rows(k, t):
        kx, kz = 2 * k + t // 4, t % 4 // 2
        pieces = []
        for e in range(2):
            ky = 2 * (t % 2) + e
            pieces += [kw0[ky, kx, kz], kw1[kx, ky, kz]]
        return pieces

    for k in range(2):
        for t in range(0, 8, 2):
            both = jnp.concatenate(head_rows(k, t) + head_rows(k, t + 1), axis=0)
            both = nt_dot(scaled, both)
            kvf[k * 8 + t] = both[:, :128]
            kvf[k * 8 + t + 1] = both[:, 128:]

    for j in range(4):
        for k in range(2):
            cs[j, k] = kvf[k * 8 + j * 2 + oc].astype(BF16)
    go("c", cs, cr, c=oc)
    arrived("c", cr)

    def term(j, k):
        return kvf[k * 8 + j * 2 + c] + cr[j, k].astype(F32)

    for k in range(2):
        ks[0, k] = term(far, k).astype(BF16)
    go("z0", ks.at[0, 0], ka.at[0], zh=right)
    go("z1", ks.at[0, 1], ka.at[1], zh=left)
    arrived("z0", ka.at[0])
    ks[1, 0] = (term(right, 0) + ka[0].astype(F32)).astype(BF16)
    ks[1, 1] = term(right, 1).astype(BF16)
    go("z2", ks.at[1], kb.at[0], zh=right)
    arrived("z1", ka.at[1])
    ks[2, 0] = term(left, 0).astype(BF16)
    ks[2, 1] = (term(left, 1) + ka[1].astype(F32)).astype(BF16)
    go("z3", ks.at[2], kb.at[1], zh=left)
    for dzh, dc in others:
        arrived(("q", dzh, dc), ssr.at[mod(zh + 4 - dzh, 4) * 2 + mod(c + dc, 2)])
    total = jnp.sum(ssr[...], axis=0)[0:1]
    factor = lax.rsqrt(jnp.broadcast_to(total, (128, 128)) / D + 1e-6)
    factor = jnp.transpose(factor)
    arrived("z2", kb.at[0])
    arrived("z3", kb.at[1])
    for k in range(2):
        done = term(zh, k) + kb[0, k].astype(F32) + kb[1, k].astype(F32)
        vis[y, zl, k] = (done * factor).astype(BF16)

    first = vis.at[y, zl]
    go("v0", first, first, zl=ozl)
    go("v1", first, first, y=up)
    go("v2", first, first, y=down)
    second = vis.at[y, ozl]
    arrived("v0", second)
    go("v3", second, second, y=up)
    go("v4", second, second, y=down)
    below = vis.at[down, zl]
    arrived("v1", below)
    go("v5", below, below, y=up)
    above = vis.at[up, ozl]
    arrived("v4", above)
    go("v6", above, above, y=down)
    arrived("v2", vis.at[up, zl])
    arrived("v3", vis.at[down, ozl])
    arrived("v5", vis.at[across, zl])
    arrived("v6", vis.at[across, ozl])
    for copy in sends:
        copy.wait_send()
    result = pltpu.make_async_copy(vis, vis_out, w_sem.at[0])
    result.start()
    result.wait()


def visual_keys_values(packed, wo, gain, live, merger, kvw, lm_gain):
    dma = pltpu.SemaphoreType.DMA
    vmem = pl.BlockSpec(memory_space=pltpu.VMEM)
    hbm = pl.BlockSpec(memory_space=pl.ANY)
    return pl.pallas_call(
        front_kernel,
        out_shape=jax.ShapeDtypeStruct((4, 2, 2, 128, 128), BF16),
        in_specs=[vmem, hbm, vmem, vmem, vmem, vmem, vmem],
        out_specs=hbm,
        scratch_shapes=[
            pltpu.VMEM((4, 16, 64, PACKED), BF16),
            pltpu.VMEM((1024, PACKED), BF16),
            pltpu.VMEM((1024, PACKED), F32),
            pltpu.VMEM((1024, HD), F32),
            pltpu.VMEM((16, 64, HD), BF16),
            pltpu.VMEM((16, 64, HD), BF16),
            pltpu.VMEM((16, HD, VIT_D), BF16),
            pltpu.VMEM((64 * VIT_D // HD, HD), F32),
            pltpu.VMEM((4, 16, VIT_D), BF16),
            pltpu.VMEM((4, 16, VIT_D), BF16),
            pltpu.VMEM((8, 4, 16, VIT_D), BF16),
            pltpu.VMEM((4, 2, 160, 1024), BF16),
            pltpu.VMEM((4, 4, 2, 32, 1024), BF16),
            pltpu.VMEM((4, 4, 2, 32, 1024), BF16),
            pltpu.VMEM((3, 128, 1024), BF16),
            pltpu.VMEM((2, 64, 1024), BF16),
            pltpu.VMEM((2, 128, 1024), BF16),
            pltpu.VMEM((16, 128, 128), F32),
            pltpu.VMEM((4, 2, 128, 128), BF16),
            pltpu.VMEM((4, 2, 128, 128), BF16),
            pltpu.VMEM((3, 2, 128, 128), BF16),
            pltpu.VMEM((2, 128, 128), BF16),
            pltpu.VMEM((2, 2, 128, 128), BF16),
            pltpu.VMEM((8, 8, 128), F32),
            pltpu.VMEM((4, 2, 2, 128, 128), BF16),
            dma((16,)), dma((16,)), dma((16,)), dma((160,)), dma((160,)),
        ],
        compiler_params=pltpu.CompilerParams(
            collective_id=0, has_side_effects=True, vmem_limit_bytes=48 * 2**20
        ),
        cost_estimate=pl.CostEstimate(
            flops=60_000_000_000, bytes_accessed=8_000_000, transcendentals=4_200_000
        ),
        name="front",
    )(packed, wo, gain, live, merger, kvw, lm_gain)


ROWS = 256


def lm_kernel(q, vis, span, bias, out):
    tile = pl.program_id(0)
    scale = HD**-0.5 * LOG2E
    ones = jnp.ones((1536, HD), BF16)
    keys = vis[:, :, 0].reshape(1024, HD)
    values = vis[:, :, 1].reshape(1024, HD)
    query = q[...]
    far = nt_dot(query, keys) + bias[...]
    near = nt_dot(query, span[0])
    token = (tile * ROWS + lax.broadcasted_iota(jnp.int32, (ROWS, 512), 0)) // 8
    place = lax.broadcasted_iota(jnp.int32, (ROWS, 512), 1)
    near = jnp.where(place <= token, near, MASKED)
    top = jnp.maximum(jnp.max(far, axis=1, keepdims=True), jnp.max(near, axis=1, keepdims=True))
    far = jnp.exp2((far - top) * scale).astype(BF16)
    near = jnp.exp2((near - top) * scale).astype(BF16)
    total = jnp.dot(
        far, jnp.concatenate([values, ones[:1024]], axis=1), preferred_element_type=F32
    ) + jnp.dot(near, jnp.concatenate([span[1], ones[:512]], axis=1), preferred_element_type=F32)
    out[...] = (total[:, :HD] / total[:, HD : HD + 1]).astype(BF16)


def lm_attention(q, vis, span, bias):
    whole = lambda *shape: pl.BlockSpec(shape, lambda i: (0,) * len(shape))
    rows = q.shape[0]
    return pl.pallas_call(
        lm_kernel,
        out_shape=jax.ShapeDtypeStruct((rows, HD), BF16),
        grid=(rows // ROWS,),
        in_specs=[
            pl.BlockSpec((ROWS, HD), lambda i: (i, 0)),
            whole(4, 2, 2, 128, 128),
            whole(2, 512, HD),
            whole(1, 1024),
        ],
        out_specs=pl.BlockSpec((ROWS, HD), lambda i: (i, 0)),
        compiler_params=pltpu.CompilerParams(vmem_limit_bytes=40 * 2**20),
        name="lm",
    )(q, vis, span, bias)


def pack_patches(vit_qkv, patch_total, first_patch):
    rows = vit_qkv.shape[1]
    split = vit_qkv[0].reshape(rows, 3, VIT_HEADS, VIT_HDIM).transpose(1, 2, 0, 3)
    ids = first_patch + jnp.arange(rows, dtype=jnp.int32)
    live = ids < patch_total
    mask = jnp.broadcast_to(
        jnp.where(live, 0.0, MASKED).astype(BF16)[None, :, None], (VIT_HEADS, rows, 1)
    )
    one = jnp.ones((VIT_HEADS, rows, 1), BF16)
    rest = jnp.zeros((VIT_HEADS, rows, PACKED - QUERY_AT - VIT_HDIM), BF16)
    packed = jnp.concatenate([split[2], one, mask, split[1], split[0], rest], axis=-1)
    return packed, live.astype(F32)[:, None]


def local(
    vit_qkv,
    patch_counts,
    vit_out_weight,
    vit_norm_gain,
    merger_weight,
    lm_norm_gain,
    kv_weight,
    queries,
    span_kv,
):
    patch_total = patch_counts[0]
    seq = lax.axis_index(SEQ)
    tp = lax.axis_index(TP)
    packed, live = pack_patches(vit_qkv, patch_total, (seq * 8 + tp) * vit_qkv.shape[1])
    vis = visual_keys_values(
        packed, vit_out_weight, vit_norm_gain[None], live,
        merger_weight, kv_weight.T, lm_norm_gain[None],
    )
    key = jnp.arange(1024, dtype=jnp.int32)
    block, r = key // 128, key % 128
    token = (((block % 2) * 4 + r // 16 % 4) * 8 + (block // 2) * 2 + r // 64) * 16 + r % 16
    bias = jnp.where(token < patch_total // 4, 0.0, MASKED)[None].astype(F32)
    rows = queries.shape[1] * queries.shape[2]
    span = span_kv[0, :, :, 0].transpose(1, 0, 2)
    out = lm_attention(queries.reshape(rows, HD), vis, span, bias)
    return out.reshape(queries.shape)


def solution(mesh):
    fine = Mesh(mesh.devices.reshape(4, 2, 4, 4, 2), ("x", "zl", "y", "zh", "c"))
    placed = (
        P("x", (*SEQ, *TP), None, None),
        P("x"),
        P(),
        P(),
        P(IMG_SEQ, TP),
        P(TP),
        P(TP, IMG_SEQ),
        P("x", SEQ, TP, None),
        P("x", SEQ, None, TP, None),
    )
    return jax.shard_map(
        local, mesh=fine, in_specs=placed, out_specs=P("x", SEQ, TP, None), check_vma=False
    )
```

```python
import jax
import jax.numpy as jnp
from jax import lax
from jax.experimental import pallas as pl
from jax.experimental.pallas import tpu as pltpu
from jax.sharding import Mesh
from jax.sharding import PartitionSpec as P

VIT_D = 1280
VIT_HEADS = 16
VIT_HDIM = 80
D = 8192
HQ = 64
KVH = 8
HD = 128
SEQ = ("zl", "y")
TP = ("zh", "c")
IMG_SEQ = ("x", "zl", "y")
MASKED = -1e30
LOG2E = 1.4426950408889634
F32 = jnp.float32
BF16 = jnp.bfloat16

LOW = 16
ONE_AT, MASK_AT, KEY_AT, QUERY_AT, PACKED = 80, 81, 82, 162, 256
RING_ORDER = (0, 1, 7, 2, 6, 3, 5, 4)


def remote(src, dst, send_sem, recv_sem, **device):
    return pltpu.make_async_remote_copy(
        src_ref=src,
        dst_ref=dst,
        send_sem=send_sem,
        recv_sem=recv_sem,
        device_id=device,
        device_id_type=pl.DeviceIdType.MESH,
    )


def mod(a, n):
    return lax.rem(a, n)


def meet(peers):
    barrier = pltpu.get_barrier_semaphore()
    for device in peers:
        pl.semaphore_signal(
            barrier, inc=1, device_id=device, device_id_type=pl.DeviceIdType.MESH
        )
    pl.semaphore_wait(barrier, len(peers))


def nt_dot(a, b):
    return lax.dot_general(a, b, (((1,), (1,)), ((), ())), preferred_element_type=F32)


def front_kernel(
    packed, wo, gain, live, merger, kvw, lm_gain, vis_out,
    kv, qp, acc, peak, back, att, wov, nf, slab, mid, tok,
    mw, kw0, kw1, sb, ra, rb, kvf, cs, cr, ks, ka, kb, ssr, vis,
    w_sem, sent, got,
):
    x, y, zh, zl, c = (lax.axis_index(a) for a in ("x", "y", "zh", "zl", "c"))
    z = zh * 2 + zl
    me = z * 2 + c
    up, down, across = mod(y + 1, 4), mod(y + 3, 4), mod(y + 2, 4)
    right, left, far = mod(zh + 1, 4), mod(zh + 3, 4), mod(zh + 2, 4)
    east, west, xfar = mod(x + 1, 4), mod(x + 3, 4), mod(x + 2, 4)
    oc, ozl = 1 - c, 1 - zl

    def place(dz, dc):
        other = mod(z + dz, 8)
        return other, mod(c + dc, 2)

    def device_of(other_z, other_c):
        return {"zh": lax.div(other_z, 2), "zl": mod(other_z, 2), "c": other_c}

    order = [(dz, dc) for dz in RING_ORDER for dc in range(2)]
    peers = [device_of(*place(dz, dc)) for dz, dc in order if (dz, dc) != (0, 0)]
    peers += [{"y": up}, {"y": down}, {"y": across}, {"x": east}, {"x": west}]
    meet(peers)

    numbers, sends = {}, []

    def number(name):
        return numbers.setdefault(name, len(numbers))

    def go(name, src, dst, **device):
        k = number(name)
        copy = remote(src, dst, sent.at[k], got.at[k], **device)
        copy.start()
        sends.append(copy)

    def arrived(name, ref):
        k = number(name)
        remote(ref, ref, sent.at[k], got.at[k], y=up).wait_recv()

    for dz in (4, 3, 5, 2, 6, 1, 7, 0):
        for dc in range(2):
            if (dz, dc) != (0, 0):
                oz, oc_ = place(dz, dc)
                go(("a", dz, dc), packed.at[oz * 2 + oc_], kv.at[y, me], **device_of(oz, oc_))
    weights = []
    for h in range(VIT_HEADS):
        copy = pltpu.make_async_copy(
            wo.at[pl.ds(h * VIT_HDIM, VIT_HDIM)], wov.at[h, pl.ds(0, VIT_HDIM)], w_sem.at[h]
        )
        copy.start()
        weights.append(copy)

    low, high = pl.ds(0, LOW), pl.ds(LOW, 64 - LOW)
    go(("k0", "e", 0), kvw.at[low], kw0.at[y, x, zl], x=east)
    go(("k0", "w", 0), kvw.at[low], kw0.at[y, x, zl], x=west)
    go(("w", "e", 0), merger, mw.at[x, zl], x=east)
    go(("w", "w", 0), merger, mw.at[x, zl], x=west)
    go(("k0", "z"), kvw.at[low], kw0.at[y, x, zl], zl=ozl)
    go(("k1", "z"), kvw.at[high], kw1.at[x, y, zl], zl=ozl)
    go(("w", "z"), merger, mw.at[x, zl], zl=ozl)
    kv[y, me] = packed[me]
    mw[x, zl] = merger[...]
    kw0[y, x, zl] = kvw[0:LOW]
    kw1[x, y, zl] = kvw[LOW:64]
    for h in range(VIT_HEADS):
        wov[h, VIT_HDIM:, :] = jnp.zeros((HD - VIT_HDIM, VIT_D), BF16)

    def source_of(dz, dc):
        return mod(z + 8 - dz, 8) * 2 + mod(c + dc, 2)

    for i, (dz, dc) in enumerate(order):
        source = source_of(dz, dc)
        if i == 0:
            block = packed.at[me]
        else:
            block = kv.at[y, source]
            arrived(("a", dz, dc), block)
        go(("y1", 0, i), block, kv.at[y, source], y=up)
        go(("y1", 1, i), block, kv.at[y, source], y=down)

    row = lax.broadcasted_iota(jnp.int32, (PACKED, PACKED), 0)
    col = lax.broadcasted_iota(jnp.int32, (PACKED, PACKED), 1)
    moved = (col >= KEY_AT) & (col < QUERY_AT) & (row == col + (QUERY_AT - KEY_AT))
    pick = moved | ((col == MASK_AT) & (row == ONE_AT))
    pick = jnp.where(pick, 1.0, 0.0).astype(BF16)
    scale = VIT_HDIM**-0.5 * LOG2E

    def rows_of(tile):
        return pl.ds(tile * 256 if isinstance(tile, int) else pl.multiple_of(tile * 256, 256), 256)

    def score(tile, block, first):
        rows = rows_of(tile)
        scores = nt_dot(qp[rows, :], block)
        top = jnp.max(scores, axis=1, keepdims=True)
        if first:
            return scores, top, None
        old = peak[rows, :][:, :1]
        return scores, jnp.maximum(old, top), old

    def blend(tile, block, scores, top, old):
        rows = rows_of(tile)
        weights = jnp.exp2((scores - top) * scale)
        total = jnp.dot(weights.astype(BF16), block, preferred_element_type=F32)
        if old is not None:
            total += acc[rows, :] * jnp.exp2((old - top) * scale)
        peak[rows, :] = jnp.broadcast_to(top, (256, HD))
        return total

    def whole(slot, first, tiles=(0, 1, 2, 3), store=None):
        block = kv[slot].reshape(1024, PACKED)
        ready = score(tiles[0], block, first)
        for t, tile in enumerate(tiles):
            following = score(tiles[t + 1], block, first) if t < 3 else None
            total = blend(tile, block, *ready)
            if store is None:
                acc[rows_of(tile), :] = total
            else:
                store(t, tile, total)
            ready = following

    qp[...] = jnp.dot(
        kv[y].reshape(1024, PACKED), pick, preferred_element_type=F32
    ).astype(BF16)
    whole(y, True)

    arrived(("k0", "z"), kw0.at[y, x, ozl])
    go(("k0", "e", 1), kw0.at[y, x, ozl], kw0.at[y, x, ozl], x=east)
    go(("k0", "w", 1), kw0.at[y, x, ozl], kw0.at[y, x, ozl], x=west)
    arrived(("k1", "z"), kw1.at[x, y, ozl])

    def piece(row, k):
        block = kw1.at[x, row]
        go(("k1", "e", k), block, block, x=east)
        go(("k1", "w", k), block, block, x=west)

    piece(y, 0)

    for i, (dz, dc) in enumerate(order):
        way, origin, target = ((0, down, up), (1, up, down))[i % 2]
        block = kv.at[origin, source_of(dz, dc)]
        arrived(("y1", way, i), block)
        go(("y2", i), block, block, y=target)
    go(("k1", "u"), kw1.at[x, y], kw1.at[x, y], y=up)
    go(("k1", "d"), kw1.at[x, y], kw1.at[x, y], y=down)
    for i, (dz, dc) in enumerate(order):
        way, origin = ((1, up), (0, down))[i % 2]
        arrived(("y1", way, i), kv.at[origin, source_of(dz, dc)])

    whole(down, False)
    arrived(("w", "z"), mw.at[x, ozl])
    go(("w", "e", 1), mw.at[x, ozl], mw.at[x, ozl], x=east)
    go(("w", "w", 1), mw.at[x, ozl], mw.at[x, ozl], x=west)
    arrived(("k0", "e", 0), kw0.at[y, west, zl])
    go(("k0", "e", 2), kw0.at[y, west, zl], kw0.at[y, west, zl], x=east)
    arrived(("w", "e", 0), mw.at[west, zl])
    go(("w", "e", 2), mw.at[west, zl], mw.at[west, zl], x=east)
    whole(up, False)
    arrived(("k0", "w", 1), kw0.at[y, east, ozl])
    go(("k0", "w", 2), kw0.at[y, east, ozl], kw0.at[y, east, ozl], x=west)
    for i, (dz, dc) in enumerate(order):
        arrived(("y2", i), kv.at[across, source_of(dz, dc)])

    def give_back(t, tile, total):
        done = (total[:, :HD] / total[:, ONE_AT : ONE_AT + 1]).astype(BF16)
        back[pl.ds(tile * 4, 4)] = done.reshape(4, 64, HD)
        for dzl in range(2):
            for dc in range(2):
                if (t, dzl, dc) == (3, 0, 0):
                    continue
                tzl, tc = mod(zl + dzl, 2), mod(c + dc, 2)
                go(
                    ("o", t, dzl, dc), back.at[tile * 4 + tzl * 2 + tc], att.at[me],
                    zh=tile, zl=tzl, c=tc,
                )

    whole(across, False, [mod(zh + 1 + t, 4) for t in range(4)], give_back)
    att[me] = back[me]

    arrived(("w", "w", 1), mw.at[east, ozl])
    go(("w", "w", 2), mw.at[east, ozl], mw.at[east, ozl], x=west)
    for copy in weights:
        copy.wait()
    for t in range(4):
        for dzl in range(2):
            for dc in range(2):
                if (t, dzl, dc) != (3, 0, 0):
                    source = mod(zh + 3 - t, 4) * 4 + mod(zl + dzl, 2) * 2 + mod(c + dc, 2)
                    arrived(("o", t, dzl, dc), att.at[source])

    hidden = jnp.zeros((64, VIT_D), F32)
    for h in range(0, VIT_HEADS, 2):
        both = jnp.concatenate([att[h], att[h + 1]], axis=1)
        hidden += jnp.dot(
            both, wov[pl.ds(h, 2)].reshape(2 * HD, VIT_D), preferred_element_type=F32
        )
    hidden = jnp.where(live[...] > 0.0, hidden, 0.0)
    centred = hidden - jnp.mean(hidden, axis=1, keepdims=True)
    spread = jnp.mean(centred * centred, axis=1, keepdims=True)
    normed = (centred * lax.rsqrt(spread + 1e-6) * gain[...]).astype(BF16).astype(F32)
    for i in range(VIT_D // HD):
        nf[pl.ds(i * 64, 64), :] = normed[:, i * HD : (i + 1) * HD]

    lane = lax.broadcasted_iota(jnp.int32, (16, VIT_D), 1)
    quarter = [
        jnp.concatenate(
            [nf[pl.ds(i * 64 + j, 16, stride=4), :] for i in range(VIT_D // HD)], axis=1
        )
        for j in range(4)
    ]
    for part in range(4):
        out = jnp.zeros((16, VIT_D), F32)
        for j in range(4):
            for half in range(2):
                start = 320 * j + 160 * half
                origin = 640 * half + 160 * part
                shift = (start - origin) % VIT_D
                rolled = pltpu.roll(quarter[j], shift, 1) if shift else quarter[j]
                out = jnp.where((lane >= start) & (lane < start + 160), rolled, out)
        slab[part] = out.astype(BF16)
    for dy in range(1, 4):
        oy = mod(y + dy, 4)
        go(("m", dy), slab.at[oy], mid.at[y], y=oy)
    mid[y] = slab[y]

    arrived(("k1", "u"), kw1.at[x, down])
    go(("k1", "u", 2), kw1.at[x, down, 0], kw1.at[x, down, 0], y=up)
    piece(down, 1)
    arrived(("k1", "d"), kw1.at[x, up])
    go(("k1", "d", 2), kw1.at[x, up, 1], kw1.at[x, up, 1], y=down)
    piece(up, 2)
    arrived(("k0", "w", 0), kw0.at[y, east, zl])
    arrived(("k0", "e", 1), kw0.at[y, west, ozl])
    arrived(("k0", "e", 2), kw0.at[y, xfar, zl])
    arrived(("k0", "w", 2), kw0.at[y, xfar, ozl])
    go(("k0", "u"), kw0.at[y], kw0.at[y], y=up)
    go(("k0", "d"), kw0.at[y], kw0.at[y], y=down)
    for dy in range(1, 4):
        arrived(("m", dy), mid.at[mod(y + 4 - dy, 4)])

    mine = zh * 2 + c
    go("t0", mid, tok.at[mine], zh=right)
    go("t1", mid, tok.at[mine], zh=left)
    go("t2", mid, tok.at[mine], c=oc)
    tok[mine] = mid[...]
    arrived(("k1", "u", 2), kw1.at[x, across, 0])
    arrived(("k1", "d", 2), kw1.at[x, across, 1])
    piece(across, 3)

    def piece_on(k, row):
        if k < 2:
            block, way, target = kw1.at[west, row], "e", east
        else:
            block, way, target = kw1.at[east, row], "w", west
        arrived(("k1", way, k), block)
        go(("k1", way, k, 2), block, block, x=target)

    piece_on(0, y)
    here = tok.at[left * 2 + c]
    arrived("t0", here)
    go("t3", here.at[pl.ds(0, 2)], here.at[pl.ds(0, 2)], zh=right)
    go("t4", here, here, c=oc)
    here = tok.at[right * 2 + c]
    arrived("t1", here)
    go("t5", here.at[pl.ds(2, 2)], here.at[pl.ds(2, 2)], zh=left)
    go("t6", here, here, c=oc)
    first, second = (tok.at[far * 2 + c].at[pl.ds(i, 2)] for i in (0, 2))
    arrived("t3", first)
    go("t7", first, first, c=oc)
    arrived("t5", second)
    go("t8", second, second, c=oc)
    piece_on(1, down)
    piece_on(2, up)
    arrived(("k0", "u"), kw0.at[down])
    go(("k0", "u", 2), kw0.at[down, pl.ds(0, 2)], kw0.at[down, pl.ds(0, 2)], y=up)
    arrived(("k0", "d"), kw0.at[up])
    go(("k0", "d", 2), kw0.at[up, pl.ds(2, 2)], kw0.at[up, pl.ds(2, 2)], y=down)
    arrived("t2", tok.at[zh * 2 + oc])
    arrived("t4", tok.at[left * 2 + oc])
    arrived("t6", tok.at[right * 2 + oc])
    arrived("t7", tok.at[far * 2 + oc].at[pl.ds(0, 2)])
    arrived("t8", tok.at[far * 2 + oc].at[pl.ds(2, 2)])
    arrived(("w", "w", 0), mw.at[east, zl])
    arrived(("w", "e", 1), mw.at[west, ozl])
    arrived(("w", "e", 2), mw.at[xfar, zl])
    arrived(("w", "w", 2), mw.at[xfar, ozl])

    def part(index):
        rows = tok[pl.ds(index * 2, 2)].reshape(128, VIT_D)
        return jnp.dot(rows, mw[...].reshape(VIT_D, 1024), preferred_element_type=F32)

    sb[0] = part(across).astype(BF16)
    go("s0", sb.at[0, pl.ds(0, 64)], ra.at[0], y=up)
    go("s1", sb.at[0, pl.ds(64, 64)], ra.at[1], y=down)
    nxt, prv = part(up), part(down)
    arrived("s0", ra.at[0])
    sb[1, 0:64] = (nxt[0:64] + ra[0].astype(F32)).astype(BF16)
    sb[1, 64:128] = nxt[64:128].astype(BF16)
    go("s2", sb.at[1], rb.at[0], y=up)
    arrived("s1", ra.at[1])
    sb[2, 0:64] = prv[0:64].astype(BF16)
    sb[2, 64:128] = (prv[64:128] + ra[1].astype(F32)).astype(BF16)
    go("s3", sb.at[2], rb.at[1], y=down)
    own = part(y)
    piece_on(3, across)
    arrived("s2", rb.at[0])
    arrived("s3", rb.at[1])
    embedded = (own + rb[0].astype(F32) + rb[1].astype(F32)).astype(BF16).astype(F32)
    square = jnp.sum(embedded * embedded, axis=1, keepdims=True)
    turned = jnp.transpose(jnp.broadcast_to(square, (128, 128)))
    others = [(dzh, dc) for dzh in range(4) for dc in range(2) if dzh or dc]
    ssr[zh * 2 + c] = turned[0:8]
    for dzh, dc in others:
        slot = ssr.at[zh * 2 + c]
        go(("q", dzh, dc), slot, slot, zh=mod(zh + dzh, 4), c=mod(c + dc, 2))
    scaled = (embedded * lm_gain[...]).astype(BF16)
    arrived(("k0", "u", 2), kw0.at[across, pl.ds(0, 2)])
    arrived(("k0", "d", 2), kw0.at[across, pl.ds(2, 2)])
    for k, row in enumerate((y, down, up, across)):
        if k < 2:
            arrived(("k1", "w", k), kw1.at[east, row])
            arrived(("k1", "e", k, 2), kw1.at[xfar, row])
        else:
            arrived(("k1", "e", k), kw1.at[west, row])
            arrived(("k1", "w", k, 2), kw1.at[xfar, row])

    def head_rows(k, t):
        kx, kz = 2 * k + t // 4, t % 4 // 2
        pieces = []
        for e in range(2):
            ky = 2 * (t % 2) + e
            pieces += [kw0[ky, kx, kz], kw1[kx, ky, kz]]
        return pieces

    for k in range(2):
        for t in range(0, 8, 2):
            both = jnp.concatenate(head_rows(k, t) + head_rows(k, t + 1), axis=0)
            both = nt_dot(scaled, both)
            kvf[k * 8 + t] = both[:, :128]
            kvf[k * 8 + t + 1] = both[:, 128:]

    for j in range(4):
        for k in range(2):
            cs[j, k] = kvf[k * 8 + j * 2 + oc].astype(BF16)
    go("c", cs, cr, c=oc)
    arrived("c", cr)

    def term(j, k):
        return kvf[k * 8 + j * 2 + c] + cr[j, k].astype(F32)

    for k in range(2):
        ks[0, k] = term(far, k).astype(BF16)
    go("z0", ks.at[0, 0], ka.at[0], zh=right)
    go("z1", ks.at[0, 1], ka.at[1], zh=left)
    arrived("z0", ka.at[0])
    ks[1, 0] = (term(right, 0) + ka[0].astype(F32)).astype(BF16)
    ks[1, 1] = term(right, 1).astype(BF16)
    go("z2", ks.at[1], kb.at[0], zh=right)
    arrived("z1", ka.at[1])
    ks[2, 0] = term(left, 0).astype(BF16)
    ks[2, 1] = (term(left, 1) + ka[1].astype(F32)).astype(BF16)
    go("z3", ks.at[2], kb.at[1], zh=left)
    for dzh, dc in others:
        arrived(("q", dzh, dc), ssr.at[mod(zh + 4 - dzh, 4) * 2 + mod(c + dc, 2)])
    total = jnp.sum(ssr[...], axis=0)[0:1]
    factor = lax.rsqrt(jnp.broadcast_to(total, (128, 128)) / D + 1e-6)
    factor = jnp.transpose(factor)
    arrived("z2", kb.at[0])
    arrived("z3", kb.at[1])
    for k in range(2):
        done = term(zh, k) + kb[0, k].astype(F32) + kb[1, k].astype(F32)
        vis[y, zl, k] = (done * factor).astype(BF16)

    first = vis.at[y, zl]
    go("v0", first, first, zl=ozl)
    go("v1", first, first, y=up)
    go("v2", first, first, y=down)
    second = vis.at[y, ozl]
    arrived("v0", second)
    go("v3", second, second, y=up)
    go("v4", second, second, y=down)
    below = vis.at[down, zl]
    arrived("v1", below)
    go("v5", below, below, y=up)
    above = vis.at[up, ozl]
    arrived("v4", above)
    go("v6", above, above, y=down)
    arrived("v2", vis.at[up, zl])
    arrived("v3", vis.at[down, ozl])
    arrived("v5", vis.at[across, zl])
    arrived("v6", vis.at[across, ozl])
    for copy in sends:
        copy.wait_send()
    result = pltpu.make_async_copy(vis, vis_out, w_sem.at[0])
    result.start()
    result.wait()


def visual_keys_values(packed, wo, gain, live, merger, kvw, lm_gain):
    dma = pltpu.SemaphoreType.DMA
    vmem = pl.BlockSpec(memory_space=pltpu.VMEM)
    hbm = pl.BlockSpec(memory_space=pl.ANY)
    return pl.pallas_call(
        front_kernel,
        out_shape=jax.ShapeDtypeStruct((4, 2, 2, 128, 128), BF16),
        in_specs=[vmem, pl.BlockSpec(memory_space=pltpu.HBM), vmem, vmem, vmem, vmem, vmem],
        out_specs=hbm,
        scratch_shapes=[
            pltpu.VMEM((4, 16, 64, PACKED), BF16),
            pltpu.VMEM((1024, PACKED), BF16),
            pltpu.VMEM((1024, PACKED), F32),
            pltpu.VMEM((1024, HD), F32),
            pltpu.VMEM((16, 64, HD), BF16),
            pltpu.VMEM((16, 64, HD), BF16),
            pltpu.VMEM((16, HD, VIT_D), BF16),
            pltpu.VMEM((64 * VIT_D // HD, HD), F32),
            pltpu.VMEM((4, 16, VIT_D), BF16),
            pltpu.VMEM((4, 16, VIT_D), BF16),
            pltpu.VMEM((8, 4, 16, VIT_D), BF16),
            pltpu.VMEM((4, 2, 160, 1024), BF16),
            pltpu.VMEM((4, 4, 2, LOW, 1024), BF16),
            pltpu.VMEM((4, 4, 2, 64 - LOW, 1024), BF16),
            pltpu.VMEM((3, 128, 1024), BF16),
            pltpu.VMEM((2, 64, 1024), BF16),
            pltpu.VMEM((2, 128, 1024), BF16),
            pltpu.VMEM((16, 128, 128), F32),
            pltpu.VMEM((4, 2, 128, 128), BF16),
            pltpu.VMEM((4, 2, 128, 128), BF16),
            pltpu.VMEM((3, 2, 128, 128), BF16),
            pltpu.VMEM((2, 128, 128), BF16),
            pltpu.VMEM((2, 2, 128, 128), BF16),
            pltpu.VMEM((8, 8, 128), F32),
            pltpu.VMEM((4, 2, 2, 128, 128), BF16),
            dma((16,)), dma((192,)), dma((192,)),
        ],
        compiler_params=pltpu.CompilerParams(
            collective_id=0, has_side_effects=True, vmem_limit_bytes=48 * 2**20
        ),
        cost_estimate=pl.CostEstimate(
            flops=60_000_000_000, bytes_accessed=8_000_000, transcendentals=4_200_000
        ),
        name="front",
    )(packed, wo, gain, live, merger, kvw, lm_gain)


ROWS = 1024
TILE = 256


def lm_kernel(q, vis, span, bias, out):
    step = pl.program_id(0)
    scale = HD**-0.5 * LOG2E
    keys = vis[:, :, 0].reshape(1024, HD)
    ones = jnp.ones((1024, HD), BF16)
    far_values = jnp.concatenate([vis[:, :, 1].reshape(1024, HD), ones], axis=1)
    near_values = jnp.concatenate([span[1], ones[:512]], axis=1)
    place = lax.broadcasted_iota(jnp.int32, (TILE, 512), 1)

    def score(i):
        query = q[pl.ds(i * TILE, TILE), :]
        far = nt_dot(query, keys) + bias[...]
        near = nt_dot(query, span[0])
        row = lax.broadcasted_iota(jnp.int32, (TILE, 512), 0)
        near = jnp.where(place <= (step * ROWS + i * TILE + row) // 8, near, MASKED)
        top = jnp.maximum(
            jnp.max(far, axis=1, keepdims=True), jnp.max(near, axis=1, keepdims=True)
        )
        return far, near, top

    def blend(i, far, near, top):
        far = jnp.exp2((far - top) * scale).astype(BF16)
        near = jnp.exp2((near - top) * scale).astype(BF16)
        total = jnp.dot(far, far_values, preferred_element_type=F32)
        total += jnp.dot(near, near_values, preferred_element_type=F32)
        out[pl.ds(i * TILE, TILE), :] = (total[:, :HD] / total[:, HD : HD + 1]).astype(BF16)

    ready = score(0)
    for i in range(ROWS // TILE):
        following = score(i + 1) if i + 1 < ROWS // TILE else None
        blend(i, *ready)
        ready = following


def lm_attention(q, vis, span, bias):
    whole = lambda *shape: pl.BlockSpec(shape, lambda i: (0,) * len(shape))
    rows = q.shape[0]
    return pl.pallas_call(
        lm_kernel,
        out_shape=jax.ShapeDtypeStruct((rows, HD), BF16),
        grid=(rows // ROWS,),
        in_specs=[
            pl.BlockSpec((ROWS, HD), lambda i: (i, 0)),
            whole(4, 2, 2, 128, 128),
            whole(2, 512, HD),
            whole(1, 1024),
        ],
        out_specs=pl.BlockSpec((ROWS, HD), lambda i: (i, 0)),
        compiler_params=pltpu.CompilerParams(vmem_limit_bytes=40 * 2**20),
        name="lm",
    )(q, vis, span, bias)


def pack_patches(vit_qkv, patch_total, first_patch):
    rows = vit_qkv.shape[1]
    split = vit_qkv[0].reshape(rows, 3, VIT_HEADS, VIT_HDIM).transpose(1, 2, 0, 3)
    ids = first_patch + jnp.arange(rows, dtype=jnp.int32)
    live = ids < patch_total
    mask = jnp.broadcast_to(
        jnp.where(live, 0.0, MASKED).astype(BF16)[None, :, None], (VIT_HEADS, rows, 1)
    )
    one = jnp.ones((VIT_HEADS, rows, 1), BF16)
    rest = jnp.zeros((VIT_HEADS, rows, PACKED - QUERY_AT - VIT_HDIM), BF16)
    packed = jnp.concatenate([split[2], one, mask, split[1], split[0], rest], axis=-1)
    return packed, live.astype(F32)[:, None]


def local(
    vit_qkv,
    patch_counts,
    vit_out_weight,
    vit_norm_gain,
    merger_weight,
    lm_norm_gain,
    kv_weight,
    queries,
    span_kv,
):
    patch_total = patch_counts[0]
    seq = lax.axis_index(SEQ)
    tp = lax.axis_index(TP)
    packed, live = pack_patches(vit_qkv, patch_total, (seq * 8 + tp) * vit_qkv.shape[1])
    vis = visual_keys_values(
        packed, vit_out_weight, vit_norm_gain[None], live,
        merger_weight, kv_weight.T, lm_norm_gain[None],
    )
    key = jnp.arange(1024, dtype=jnp.int32)
    block, r = key // 128, key % 128
    token = (((block % 2) * 4 + r // 16 % 4) * 8 + (block // 2) * 2 + r // 64) * 16 + r % 16
    bias = jnp.where(token < patch_total // 4, 0.0, MASKED)[None].astype(F32)
    rows = queries.shape[1] * queries.shape[2]
    span = span_kv[0, :, :, 0].transpose(1, 0, 2)
    out = lm_attention(queries.reshape(rows, HD), vis, span, bias)
    return out.reshape(queries.shape)


def solution(mesh):
    fine = Mesh(mesh.devices.reshape(4, 2, 4, 4, 2), ("x", "zl", "y", "zh", "c"))
    placed = (
        P("x", (*SEQ, *TP), None, None),
        P("x"),
        P(),
        P(),
        P(IMG_SEQ, TP),
        P(TP),
        P(TP, IMG_SEQ),
        P("x", SEQ, TP, None),
        P("x", SEQ, None, TP, None),
    )
    return jax.shard_map(
        local, mesh=fine, in_specs=placed, out_specs=P("x", SEQ, TP, None), check_vma=False
    )
```

```python
import jax
import jax.numpy as jnp
from jax import lax
from jax.experimental import pallas as pl
from jax.experimental.pallas import tpu as pltpu
from jax.sharding import Mesh
from jax.sharding import PartitionSpec as P

VIT_D = 1280
VIT_HEADS = 16
VIT_HDIM = 80
D = 8192
HQ = 64
KVH = 8
HD = 128
SEQ = ("zl", "y")
TP = ("zh", "c")
IMG_SEQ = ("x", "zl", "y")
MASKED = -1e30
LOG2E = 1.4426950408889634
F32 = jnp.float32
BF16 = jnp.bfloat16

LOW = 16
COPIES = 124
ONE_AT, MASK_AT, KEY_AT, QUERY_AT, PACKED = 80, 81, 82, 162, 256
RING_ORDER = (0, 1, 7, 2, 6, 3, 5, 4)


def remote(src, dst, send_sem, recv_sem, **device):
    return pltpu.make_async_remote_copy(
        src_ref=src,
        dst_ref=dst,
        send_sem=send_sem,
        recv_sem=recv_sem,
        device_id=device,
        device_id_type=pl.DeviceIdType.MESH,
    )


def mod(a, n):
    return lax.rem(a, n)


def meet(peers, meanwhile):
    barrier = pltpu.get_barrier_semaphore()
    for device in peers:
        pl.semaphore_signal(
            barrier, inc=1, device_id=device, device_id_type=pl.DeviceIdType.MESH
        )
    meanwhile()
    pl.semaphore_wait(barrier, len(peers))


def nt_dot(a, b):
    return lax.dot_general(a, b, (((1,), (1,)), ((), ())), preferred_element_type=F32)


def front_kernel(
    counts, qkv, wo, gain, merger, kvw, lm_gain, queries, span, out,
    packed, kv, qp, acc, peak, back, att, wov, nf, slab, mid, tok,
    mw, kw0, kw1, sb, ra, rb, kvf, cs, cr, ks, ka, kb, ssr, vis, q, lacc, lpeak, result,
    w_sem, sent, got,
):
    x, y, zh, zl, c = (lax.axis_index(a) for a in ("x", "y", "zh", "zl", "c"))
    z = zh * 2 + zl
    me = z * 2 + c
    up, down, across = mod(y + 1, 4), mod(y + 3, 4), mod(y + 2, 4)
    right, left, far = mod(zh + 1, 4), mod(zh + 3, 4), mod(zh + 2, 4)
    east, west, xfar = mod(x + 1, 4), mod(x + 3, 4), mod(x + 2, 4)
    oc, ozl = 1 - c, 1 - zl

    def place(dz, dc):
        other = mod(z + dz, 8)
        return other, mod(c + dc, 2)

    def device_of(other_z, other_c):
        return {"zh": lax.div(other_z, 2), "zl": mod(other_z, 2), "c": other_c}

    order = [(dz, dc) for dz in RING_ORDER for dc in range(2)]
    peers = [device_of(*place(dz, dc)) for dz, dc in order if (dz, dc) != (0, 0)]
    peers += [{"y": up}, {"y": down}, {"y": across}, {"x": east}, {"x": west}]
    total_patches = counts[0]
    first_patch = ((zl * 4 + y) * 8 + zh * 2 + c) * 64
    live = first_patch + lax.broadcasted_iota(jnp.int32, (64, PACKED), 0) < total_patches
    low, high = pl.ds(0, LOW), pl.ds(LOW, 64 - LOW)

    load_q = pltpu.make_async_copy(queries, q, w_sem.at[16])
    load_q.start()
    weights = []
    for h in range(VIT_HEADS):
        copy = pltpu.make_async_copy(
            wo.at[pl.ds(h * VIT_HDIM, VIT_HDIM)], wov.at[h, pl.ds(0, VIT_HDIM)], w_sem.at[h]
        )
        copy.start()
        weights.append(copy)

    def own_part():
        column = lax.broadcasted_iota(jnp.int32, (64, PACKED), 1)
        rest = jnp.where(column == ONE_AT, 1.0, 0.0)
        rest = jnp.where((column == MASK_AT) & ~live, MASKED, rest)
        for h in range(VIT_HEADS):
            start = min(h * VIT_HDIM // HD * HD, VIT_D - PACKED)
            row = rest
            for which, at in ((2, 0), (1, KEY_AT), (0, QUERY_AT)):
                window = qkv[which, :, start : start + PACKED].astype(F32)
                shift = (at - (h * VIT_HDIM - start)) % PACKED
                if shift:
                    window = pltpu.roll(window, shift, 1)
                row = jnp.where((column >= at) & (column < at + VIT_HDIM), window, row)
            packed[h] = row.astype(BF16)
        kv[y, me] = packed[me]
        mw[x, zl] = merger[...]
        kw0[y, x, zl] = kvw[0:LOW]
        kw1[x, y, zl] = kvw[LOW:64]
        for h in range(VIT_HEADS):
            wov[h, VIT_HDIM:, :] = jnp.zeros((HD - VIT_HDIM, VIT_D), BF16)

    meet(peers, own_part)

    numbers, sends = {}, []

    def number(name):
        return numbers.setdefault(name, len(numbers))

    def go(name, src, dst, **device):
        k = number(name)
        copy = remote(src, dst, sent.at[k], got.at[k], **device)
        copy.start()
        sends.append(copy)

    def arrived(name, ref):
        k = number(name)
        remote(ref, ref, sent.at[k], got.at[k], y=up).wait_recv()

    lm_scale = HD**-0.5 * LOG2E
    lm_tiles = queries.shape[0] // 256

    def lm_rows(i):
        return pl.ds(i * 256, 256)

    def near_part():
        def near_score(i):
            extent = (i // 4 + 1) * 128
            keys = span[0, 0:extent, :]
            scores = nt_dot(q[lm_rows(i), :], keys)
            row = lax.broadcasted_iota(jnp.int32, (256, 128), 0)
            place_ = lax.broadcasted_iota(jnp.int32, (256, 128), 1)
            edge = jnp.where(
                place_ + (extent - 128) <= (i * 256 + row) // 8, scores[:, extent - 128 :], MASKED
            )
            if extent > 128:
                edge = jnp.concatenate([scores[:, : extent - 128], edge], axis=1)
            return edge, jnp.max(edge, axis=1, keepdims=True), extent

        ready = near_score(0)
        for i in range(lm_tiles):
            following = near_score(i + 1) if i + 1 < lm_tiles else None
            scores, top, extent = ready
            weights = jnp.exp2((scores - top) * lm_scale).astype(BF16)
            values = jnp.concatenate([span[1, 0:extent, :], jnp.ones((extent, HD), BF16)], axis=1)
            lacc[lm_rows(i), :] = jnp.dot(weights, values, preferred_element_type=F32)
            lpeak[lm_rows(i), :] = jnp.broadcast_to(top, (256, HD))
            ready = following

    def far_part(slots, store, between):
        keys = jnp.concatenate([vis[a, b, 0] for a, b in slots], axis=0)
        values = jnp.concatenate([vis[a, b, 1] for a, b in slots], axis=0)
        values = jnp.concatenate([values, jnp.ones((len(slots) * 128, HD), BF16)], axis=1)
        lane = lax.broadcasted_iota(jnp.int32, (1, HD), 1)

        def slot_bias(a, b):
            patch = ((b * 4 + (lane >> 4 & 3)) * 8 + a * 2 + (lane >> 6)) * 64 + (lane & 15) * 4
            return jnp.where(patch < total_patches, 0.0, MASKED)

        shift = jnp.concatenate([slot_bias(a, b) for a, b in slots], axis=1)

        def far_score(i):
            scores = nt_dot(q[lm_rows(i), :], keys) + shift
            old = lpeak[lm_rows(i), :]
            return scores, jnp.maximum(old, jnp.max(scores, axis=1, keepdims=True)), old

        ready = far_score(0)
        for i in range(lm_tiles):
            following = far_score(i + 1) if i + 1 < lm_tiles else None
            scores, top, old = ready
            spread = jnp.concatenate([top] * len(slots), axis=1)
            weights = jnp.exp2((scores - spread) * lm_scale).astype(BF16)
            total = jnp.dot(weights, values, preferred_element_type=F32)
            fade = jnp.exp2((old - top) * lm_scale)
            total += lacc[lm_rows(i), :] * jnp.concatenate([fade, fade], axis=1)
            store(i, total, top)
            between(i)
            ready = following

    for dz in (4, 3, 5, 2, 6, 1, 7, 0):
        for dc in range(2):
            if (dz, dc) != (0, 0):
                oz, oc_ = place(dz, dc)
                go(("a", dz, dc), packed.at[oz * 2 + oc_], kv.at[y, me], **device_of(oz, oc_))
    go(("k0", "e", 0), kvw.at[low], kw0.at[y, x, zl], x=east)
    go(("k0", "w", 0), kvw.at[low], kw0.at[y, x, zl], x=west)
    go(("w", "e", 0), merger, mw.at[x, zl], x=east)
    go(("w", "w", 0), merger, mw.at[x, zl], x=west)
    def blocks_of(row, dz):
        return kv.at[row, pl.ds(mod(z + 8 - dz, 8) * 2, 2)]

    def source_of(dz, dc):
        return mod(z + 8 - dz, 8) * 2 + mod(c + dc, 2)

    for i, dz in enumerate(RING_ORDER):
        for dc in range(2):
            if (dz, dc) != (0, 0):
                arrived(("a", dz, dc), kv.at[y, source_of(dz, dc)])
        blocks = blocks_of(y, dz)
        go(("y1", 0, i), blocks, blocks, y=up)
        go(("y1", 1, i), blocks, blocks, y=down)

    go(("k0", "z"), kvw.at[low], kw0.at[y, x, zl], zl=ozl)
    go(("k1", "z"), kvw.at[high], kw1.at[x, y, zl], zl=ozl)
    go(("w", "z"), merger, mw.at[x, zl], zl=ozl)
    row = lax.broadcasted_iota(jnp.int32, (PACKED, PACKED), 0)
    col = lax.broadcasted_iota(jnp.int32, (PACKED, PACKED), 1)
    moved = (col >= KEY_AT) & (col < QUERY_AT) & (row == col + (QUERY_AT - KEY_AT))
    pick = moved | ((col == MASK_AT) & (row == ONE_AT))
    pick = jnp.where(pick, 1.0, 0.0).astype(BF16)
    scale = VIT_HDIM**-0.5 * LOG2E

    def rows_of(tile):
        return pl.ds(tile * 256 if isinstance(tile, int) else pl.multiple_of(tile * 256, 256), 256)

    def score(tile, block, first):
        rows = rows_of(tile)
        scores = nt_dot(qp[rows, :], block)
        top = jnp.broadcast_to(jnp.max(scores, axis=1, keepdims=True), (256, HD))
        if first:
            return scores, top, None
        old = peak[rows, :]
        return scores, jnp.maximum(old, top), old

    def blend(tile, block, scores, top, old):
        rows = rows_of(tile)
        weights = jnp.exp2((scores - jnp.concatenate([top] * 8, axis=1)) * scale)
        total = jnp.dot(weights.astype(BF16), block, preferred_element_type=F32)
        if old is not None:
            fade = jnp.exp2((old - top) * scale)
            total += acc[rows, :] * jnp.concatenate([fade, fade], axis=1)
        peak[rows, :] = top
        return total

    def whole(slot, first, tiles=(0, 1, 2, 3), store=None):
        block = kv[slot].reshape(1024, PACKED)
        ready = score(tiles[0], block, first)
        for t, tile in enumerate(tiles):
            following = score(tiles[t + 1], block, first) if t < 3 else None
            total = blend(tile, block, *ready)
            if store is None:
                acc[rows_of(tile), :] = total
            else:
                store(t, tile, total)
            ready = following

    qp[...] = jnp.dot(
        kv[y].reshape(1024, PACKED), pick, preferred_element_type=F32
    ).astype(BF16)
    whole(y, True)

    for i, dz in enumerate(RING_ORDER):
        way, origin, target = ((0, down, up), (1, up, down))[i % 2]
        blocks = blocks_of(origin, dz)
        arrived(("y1", way, i), blocks)
        go(("y2", i), blocks, blocks, y=target)
    arrived(("k0", "z"), kw0.at[y, x, ozl])
    go(("k0", "e", 1), kw0.at[y, x, ozl], kw0.at[y, x, ozl], x=east)
    go(("k0", "w", 1), kw0.at[y, x, ozl], kw0.at[y, x, ozl], x=west)
    arrived(("k1", "z"), kw1.at[x, y, ozl])

    def piece(row, k):
        block = kw1.at[x, row]
        go(("k1", "e", k), block, block, x=east)
        go(("k1", "w", k), block, block, x=west)

    piece(y, 0)

    go(("k1", "u"), kw1.at[x, y], kw1.at[x, y], y=up)
    go(("k1", "d"), kw1.at[x, y], kw1.at[x, y], y=down)
    for i, dz in enumerate(RING_ORDER):
        way, origin = ((1, up), (0, down))[i % 2]
        arrived(("y1", way, i), blocks_of(origin, dz))

    whole(down, False)
    arrived(("w", "z"), mw.at[x, ozl])
    go(("w", "e", 1), mw.at[x, ozl], mw.at[x, ozl], x=east)
    go(("w", "w", 1), mw.at[x, ozl], mw.at[x, ozl], x=west)
    arrived(("k0", "e", 0), kw0.at[y, west, zl])
    go(("k0", "e", 2), kw0.at[y, west, zl], kw0.at[y, west, zl], x=east)
    arrived(("w", "e", 0), mw.at[west, zl])
    go(("w", "e", 2), mw.at[west, zl], mw.at[west, zl], x=east)
    whole(up, False)
    arrived(("k0", "w", 1), kw0.at[y, east, ozl])
    go(("k0", "w", 2), kw0.at[y, east, ozl], kw0.at[y, east, ozl], x=west)
    for i, dz in enumerate(RING_ORDER):
        arrived(("y2", i), blocks_of(across, dz))

    def give_back(t, tile, total):
        done = (total[:, :HD] / total[:, ONE_AT : ONE_AT + 1]).astype(BF16)
        back[pl.ds(tile * 4, 4)] = done.reshape(4, 64, HD)
        for dzl in range(2):
            for dc in range(2):
                if (t, dzl, dc) == (3, 0, 0):
                    continue
                tzl, tc = mod(zl + dzl, 2), mod(c + dc, 2)
                go(
                    ("o", t, dzl, dc), back.at[tile * 4 + tzl * 2 + tc], att.at[me],
                    zh=tile, zl=tzl, c=tc,
                )

    whole(across, False, [mod(zh + 1 + t, 4) for t in range(4)], give_back)
    att[me] = back[me]

    for copy in weights:
        copy.wait()
    for t in range(4):
        for dzl in range(2):
            for dc in range(2):
                if (t, dzl, dc) != (3, 0, 0):
                    source = mod(zh + 3 - t, 4) * 4 + mod(zl + dzl, 2) * 2 + mod(c + dc, 2)
                    arrived(("o", t, dzl, dc), att.at[source])

    hidden = jnp.zeros((64, VIT_D), F32)
    for h in range(0, VIT_HEADS, 2):
        both = jnp.concatenate([att[h], att[h + 1]], axis=1)
        hidden += jnp.dot(
            both, wov[pl.ds(h, 2)].reshape(2 * HD, VIT_D), preferred_element_type=F32
        )
    hidden = jnp.where(live[:, :1], hidden, 0.0)
    centred = hidden - jnp.mean(hidden, axis=1, keepdims=True)
    spread = jnp.mean(centred * centred, axis=1, keepdims=True)
    normed = (centred * lax.rsqrt(spread + 1e-6) * gain[...]).astype(BF16).astype(F32)
    for i in range(VIT_D // HD):
        nf[pl.ds(i * 64, 64), :] = normed[:, i * HD : (i + 1) * HD]

    lane = lax.broadcasted_iota(jnp.int32, (16, VIT_D), 1)
    quarter = [
        jnp.concatenate(
            [nf[pl.ds(i * 64 + j, 16, stride=4), :] for i in range(VIT_D // HD)], axis=1
        )
        for j in range(4)
    ]
    for part in range(4):
        laid = jnp.zeros((16, VIT_D), F32)
        for j in range(4):
            for half in range(2):
                start = 320 * j + 160 * half
                origin = 640 * half + 160 * part
                shift = (start - origin) % VIT_D
                rolled = pltpu.roll(quarter[j], shift, 1) if shift else quarter[j]
                laid = jnp.where((lane >= start) & (lane < start + 160), rolled, laid)
        slab[part] = laid.astype(BF16)
    for dy in range(1, 4):
        oy = mod(y + dy, 4)
        go(("m", dy), slab.at[oy], mid.at[y], y=oy)
    mid[y] = slab[y]

    arrived(("w", "w", 1), mw.at[east, ozl])
    go(("w", "w", 2), mw.at[east, ozl], mw.at[east, ozl], x=west)
    arrived(("k1", "u"), kw1.at[x, down])
    go(("k1", "u", 2), kw1.at[x, down, 0], kw1.at[x, down, 0], y=up)
    piece(down, 1)
    arrived(("k1", "d"), kw1.at[x, up])
    go(("k1", "d", 2), kw1.at[x, up, 1], kw1.at[x, up, 1], y=down)
    piece(up, 2)
    arrived(("k0", "w", 0), kw0.at[y, east, zl])
    arrived(("k0", "e", 1), kw0.at[y, west, ozl])
    arrived(("k0", "e", 2), kw0.at[y, xfar, zl])
    arrived(("k0", "w", 2), kw0.at[y, xfar, ozl])
    go(("k0", "u"), kw0.at[y], kw0.at[y], y=up)
    go(("k0", "d"), kw0.at[y], kw0.at[y], y=down)
    for dy in range(1, 4):
        arrived(("m", dy), mid.at[mod(y + 4 - dy, 4)])

    mine = zh * 2 + c
    go("t0", mid, tok.at[mine], zh=right)
    go("t1", mid, tok.at[mine], zh=left)
    go("t2", mid, tok.at[mine], c=oc)
    tok[mine] = mid[...]
    load_q.wait()
    near_part()
    arrived(("k1", "u", 2), kw1.at[x, across, 0])
    arrived(("k1", "d", 2), kw1.at[x, across, 1])
    piece(across, 3)

    def piece_on(k, row):
        if k < 2:
            block, way, target = kw1.at[west, row], "e", east
        else:
            block, way, target = kw1.at[east, row], "w", west
        arrived(("k1", way, k), block)
        go(("k1", way, k, 2), block, block, x=target)

    piece_on(0, y)
    here = tok.at[left * 2 + c]
    arrived("t0", here)
    go("t3", here.at[pl.ds(0, 2)], here.at[pl.ds(0, 2)], zh=right)
    go("t4", here, here, c=oc)
    here = tok.at[right * 2 + c]
    arrived("t1", here)
    go("t5", here.at[pl.ds(2, 2)], here.at[pl.ds(2, 2)], zh=left)
    go("t6", here, here, c=oc)
    first, second = (tok.at[far * 2 + c].at[pl.ds(i, 2)] for i in (0, 2))
    arrived("t3", first)
    go("t7", first, first, c=oc)
    arrived("t5", second)
    go("t8", second, second, c=oc)
    piece_on(1, down)
    piece_on(2, up)
    arrived(("k0", "u"), kw0.at[down])
    go(("k0", "u", 2), kw0.at[down, pl.ds(0, 2)], kw0.at[down, pl.ds(0, 2)], y=up)
    arrived(("k0", "d"), kw0.at[up])
    go(("k0", "d", 2), kw0.at[up, pl.ds(2, 2)], kw0.at[up, pl.ds(2, 2)], y=down)
    arrived("t2", tok.at[zh * 2 + oc])
    arrived("t4", tok.at[left * 2 + oc])
    arrived("t6", tok.at[right * 2 + oc])
    arrived("t7", tok.at[far * 2 + oc].at[pl.ds(0, 2)])
    arrived("t8", tok.at[far * 2 + oc].at[pl.ds(2, 2)])
    arrived(("w", "w", 0), mw.at[east, zl])
    arrived(("w", "e", 1), mw.at[west, ozl])
    arrived(("w", "e", 2), mw.at[xfar, zl])
    arrived(("w", "w", 2), mw.at[xfar, ozl])

    def part(index):
        rows = tok[pl.ds(index * 2, 2)].reshape(128, VIT_D)
        return jnp.dot(rows, mw[...].reshape(VIT_D, 1024), preferred_element_type=F32)

    sb[0] = part(across).astype(BF16)
    go("s0", sb.at[0, pl.ds(0, 64)], ra.at[0], y=up)
    go("s1", sb.at[0, pl.ds(64, 64)], ra.at[1], y=down)
    nxt, prv = part(up), part(down)
    arrived("s0", ra.at[0])
    sb[1, 0:64] = (nxt[0:64] + ra[0].astype(F32)).astype(BF16)
    sb[1, 64:128] = nxt[64:128].astype(BF16)
    go("s2", sb.at[1], rb.at[0], y=up)
    arrived("s1", ra.at[1])
    sb[2, 0:64] = prv[0:64].astype(BF16)
    sb[2, 64:128] = (prv[64:128] + ra[1].astype(F32)).astype(BF16)
    go("s3", sb.at[2], rb.at[1], y=down)
    own = part(y)
    piece_on(3, across)
    arrived("s2", rb.at[0])
    arrived("s3", rb.at[1])
    embedded = (own + rb[0].astype(F32) + rb[1].astype(F32)).astype(BF16).astype(F32)
    square = jnp.sum(embedded * embedded, axis=1, keepdims=True)
    turned = jnp.transpose(jnp.broadcast_to(square, (128, 128)))
    others = [(dzh, dc) for dzh in range(4) for dc in range(2) if dzh or dc]
    ssr[zh * 2 + c] = turned[0:8]
    for dzh, dc in others:
        slot = ssr.at[zh * 2 + c]
        go(("q", dzh, dc), slot, slot, zh=mod(zh + dzh, 4), c=mod(c + dc, 2))
    scaled = (embedded * lm_gain[...]).astype(BF16)
    arrived(("k0", "u", 2), kw0.at[across, pl.ds(0, 2)])
    arrived(("k0", "d", 2), kw0.at[across, pl.ds(2, 2)])
    for k, row in enumerate((y, down, up, across)):
        if k < 2:
            arrived(("k1", "w", k), kw1.at[east, row])
            arrived(("k1", "e", k, 2), kw1.at[xfar, row])
        else:
            arrived(("k1", "e", k), kw1.at[west, row])
            arrived(("k1", "w", k, 2), kw1.at[xfar, row])

    def head_rows(k, t):
        kx, kz = 2 * k + t // 4, t % 4 // 2
        pieces = []
        for e in range(2):
            ky = 2 * (t % 2) + e
            pieces += [kw0[ky, kx, kz], kw1[kx, ky, kz]]
        return pieces

    for k in range(2):
        for t in range(0, 8, 2):
            both = jnp.concatenate(head_rows(k, t) + head_rows(k, t + 1), axis=0)
            both = nt_dot(scaled, both)
            kvf[k * 8 + t] = both[:, :128]
            kvf[k * 8 + t + 1] = both[:, 128:]

    for j in range(4):
        for k in range(2):
            cs[j, k] = kvf[k * 8 + j * 2 + oc].astype(BF16)
    go("c", cs, cr, c=oc)
    arrived("c", cr)

    def term(j, k):
        return kvf[k * 8 + j * 2 + c] + cr[j, k].astype(F32)

    for k in range(2):
        ks[0, k] = term(far, k).astype(BF16)
    go("z0", ks.at[0, 0], ka.at[0], zh=right)
    go("z1", ks.at[0, 1], ka.at[1], zh=left)
    arrived("z0", ka.at[0])
    ks[1, 0] = (term(right, 0) + ka[0].astype(F32)).astype(BF16)
    ks[1, 1] = term(right, 1).astype(BF16)
    go("z2", ks.at[1], kb.at[0], zh=right)
    arrived("z1", ka.at[1])
    ks[2, 0] = term(left, 0).astype(BF16)
    ks[2, 1] = (term(left, 1) + ka[1].astype(F32)).astype(BF16)
    go("z3", ks.at[2], kb.at[1], zh=left)
    for dzh, dc in others:
        arrived(("q", dzh, dc), ssr.at[mod(zh + 4 - dzh, 4) * 2 + mod(c + dc, 2)])
    total = jnp.sum(ssr[...], axis=0)[0:1]
    factor = lax.rsqrt(jnp.broadcast_to(total, (128, 128)) / D + 1e-6)
    factor = jnp.transpose(factor)
    arrived("z2", kb.at[0])
    arrived("z3", kb.at[1])
    for k in range(2):
        done = term(zh, k) + kb[0, k].astype(F32) + kb[1, k].astype(F32)
        vis[y, zl, k] = (done * factor).astype(BF16)

    first = vis.at[y, zl]
    go("v0", first, first, zl=ozl)
    go("v1", first, first, y=up)
    go("v2", first, first, y=down)
    second = vis.at[y, ozl]
    arrived("v0", second)
    go("v3", second, second, y=up)
    go("v4", second, second, y=down)
    below = vis.at[down, zl]
    arrived("v1", below)
    go("v5", below, below, y=up)
    arrived("v2", vis.at[up, zl])

    def keep(i, total, top):
        lacc[lm_rows(i), :] = total
        lpeak[lm_rows(i), :] = top

    def pass_up(i):
        if i == 3:
            above = vis.at[up, ozl]
            arrived("v4", above)
            go("v6", above, above, y=down)

    far_part([(y, zl), (y, ozl), (down, zl), (up, zl)], keep, pass_up)
    arrived("v3", vis.at[down, ozl])
    arrived("v5", vis.at[across, zl])
    arrived("v6", vis.at[across, ozl])
    stores = []

    def finish(i, total, top):
        result[lm_rows(i), :] = (total[:, :HD] / total[:, HD:]).astype(BF16)

    def write(i):
        if i % 4 == 3:
            rows = pl.ds((i - 3) * 256, 1024)
            copy = pltpu.make_async_copy(result.at[rows], out.at[rows], w_sem.at[17 + i // 4])
            copy.start()
            stores.append(copy)

    far_part([(down, ozl), (up, ozl), (across, zl), (across, ozl)], finish, write)
    assert len(numbers) == COPIES, len(numbers)
    for copy in sends:
        copy.wait_send()
    for copy in stores:
        copy.wait()


def attend(counts, qkv, wo, gain, merger, kvw, lm_gain, queries, span):
    dma = pltpu.SemaphoreType.DMA
    vmem = pl.BlockSpec(memory_space=pltpu.VMEM)
    hbm = pl.BlockSpec(memory_space=pl.ANY)
    return pl.pallas_call(
        front_kernel,
        out_shape=jax.ShapeDtypeStruct(queries.shape, BF16),
        in_specs=[
            pl.BlockSpec(memory_space=pltpu.SMEM), vmem, hbm, vmem, vmem, vmem, vmem, hbm, vmem,
        ],
        out_specs=hbm,
        scratch_shapes=[
            pltpu.VMEM((16, 64, PACKED), BF16),
            pltpu.VMEM((4, 16, 64, PACKED), BF16),
            pltpu.VMEM((1024, PACKED), BF16),
            pltpu.VMEM((1024, PACKED), F32),
            pltpu.VMEM((1024, HD), F32),
            pltpu.VMEM((16, 64, HD), BF16),
            pltpu.VMEM((16, 64, HD), BF16),
            pltpu.VMEM((16, HD, VIT_D), BF16),
            pltpu.VMEM((64 * VIT_D // HD, HD), F32),
            pltpu.VMEM((4, 16, VIT_D), BF16),
            pltpu.VMEM((4, 16, VIT_D), BF16),
            pltpu.VMEM((8, 4, 16, VIT_D), BF16),
            pltpu.VMEM((4, 2, 160, 1024), BF16),
            pltpu.VMEM((4, 4, 2, LOW, 1024), BF16),
            pltpu.VMEM((4, 4, 2, 64 - LOW, 1024), BF16),
            pltpu.VMEM((3, 128, 1024), BF16),
            pltpu.VMEM((2, 64, 1024), BF16),
            pltpu.VMEM((2, 128, 1024), BF16),
            pltpu.VMEM((16, 128, 128), F32),
            pltpu.VMEM((4, 2, 128, 128), BF16),
            pltpu.VMEM((4, 2, 128, 128), BF16),
            pltpu.VMEM((3, 2, 128, 128), BF16),
            pltpu.VMEM((2, 128, 128), BF16),
            pltpu.VMEM((2, 2, 128, 128), BF16),
            pltpu.VMEM((8, 8, 128), F32),
            pltpu.VMEM((4, 2, 2, 128, 128), BF16),
            pltpu.VMEM((4096, HD), BF16),
            pltpu.VMEM((4096, 2 * HD), F32),
            pltpu.VMEM((4096, HD), F32),
            pltpu.VMEM((4096, HD), BF16),
            dma((21,)), dma((COPIES,)), dma((COPIES,)),
        ],
        compiler_params=pltpu.CompilerParams(
            collective_id=0, has_side_effects=True, vmem_limit_bytes=61 * 2**20
        ),
        cost_estimate=pl.CostEstimate(
            flops=60_000_000_000, bytes_accessed=8_000_000, transcendentals=4_200_000
        ),
        name="front",
    )(counts, qkv, wo, gain, merger, kvw, lm_gain, queries, span)


def local(
    vit_qkv,
    patch_counts,
    vit_out_weight,
    vit_norm_gain,
    merger_weight,
    lm_norm_gain,
    kv_weight,
    queries,
    span_kv,
):
    rows = queries.shape[1] * queries.shape[2]
    span = span_kv[0, :, :, 0].transpose(1, 0, 2)
    out = attend(
        patch_counts, vit_qkv[0].transpose(1, 0, 2), vit_out_weight, vit_norm_gain[None],
        merger_weight, kv_weight.T, lm_norm_gain[None], queries.reshape(rows, HD), span,
    )
    return out.reshape(queries.shape)


def solution(mesh):
    fine = Mesh(mesh.devices.reshape(4, 2, 4, 4, 2), ("x", "zl", "y", "zh", "c"))
    placed = (
        P("x", (*SEQ, *TP), None, None),
        P("x"),
        P(),
        P(),
        P(IMG_SEQ, TP),
        P(TP),
        P(TP, IMG_SEQ),
        P("x", SEQ, TP, None),
        P("x", SEQ, None, TP, None),
    )
    return jax.shard_map(
        local, mesh=fine, in_specs=placed, out_specs=P("x", SEQ, TP, None), check_vma=False
    )
```

```python
import jax
import jax.numpy as jnp
from jax import lax
from jax.experimental import pallas as pl
from jax.experimental.pallas import tpu as pltpu
from jax.sharding import Mesh
from jax.sharding import PartitionSpec as P

VIT_D = 1280
VIT_HEADS = 16
VIT_HDIM = 80
D = 8192
HQ = 64
KVH = 8
HD = 128
SEQ = ("zl", "y")
TP = ("zh", "c")
IMG_SEQ = ("x", "zl", "y")
MASKED = -1e30
LOG2E = 1.4426950408889634
F32 = jnp.float32
BF16 = jnp.bfloat16

LOW = 16
COPIES = 130
ONE_AT, MASK_AT, KEY_AT, QUERY_AT, PACKED = 80, 81, 82, 162, 256
RING_ORDER = (0, 1, 7, 2, 6, 3, 5, 4)


def remote(src, dst, send_sem, recv_sem, **device):
    return pltpu.make_async_remote_copy(
        src_ref=src,
        dst_ref=dst,
        send_sem=send_sem,
        recv_sem=recv_sem,
        device_id=device,
        device_id_type=pl.DeviceIdType.MESH,
    )


def mod(a, n):
    return lax.rem(a, n)


def meet(peers, meanwhile):
    barrier = pltpu.get_barrier_semaphore()
    for device in peers:
        pl.semaphore_signal(
            barrier, inc=1, device_id=device, device_id_type=pl.DeviceIdType.MESH
        )
    meanwhile()
    pl.semaphore_wait(barrier, len(peers))


def nt_dot(a, b):
    return lax.dot_general(a, b, (((1,), (1,)), ((), ())), preferred_element_type=F32)


def front_kernel(
    counts, qkv, wo, gain, merger, kvw, lm_gain, queries, span, out,
    packed, kv, qp, acc, peak, back, att, wov, nf, slab, mid, tok,
    mw, kw0, kw1, sb, ra, rb, kvf, cs, cr, ks, ka, kb, ssr, vis, q, lacc, lpeak, result,
    w_sem, sent, got,
):
    x, y, zh, zl, c = (lax.axis_index(a) for a in ("x", "y", "zh", "zl", "c"))
    z = zh * 2 + zl
    me = z * 2 + c
    up, down, across = mod(y + 1, 4), mod(y + 3, 4), mod(y + 2, 4)
    right, left, far = mod(zh + 1, 4), mod(zh + 3, 4), mod(zh + 2, 4)
    east, west, xfar = mod(x + 1, 4), mod(x + 3, 4), mod(x + 2, 4)
    oc, ozl = 1 - c, 1 - zl

    def place(dz, dc):
        other = mod(z + dz, 8)
        return other, mod(c + dc, 2)

    def device_of(other_z, other_c):
        return {"zh": lax.div(other_z, 2), "zl": mod(other_z, 2), "c": other_c}

    order = [(dz, dc) for dz in RING_ORDER for dc in range(2)]
    peers = [device_of(*place(dz, dc)) for dz, dc in order if (dz, dc) != (0, 0)]
    peers += [{"y": up}, {"y": down}, {"y": across}, {"x": east}, {"x": west}]
    total_patches = counts[0]
    first_patch = ((zl * 4 + y) * 8 + zh * 2 + c) * 64
    live = first_patch + lax.broadcasted_iota(jnp.int32, (64, PACKED), 0) < total_patches
    low, high = pl.ds(0, LOW), pl.ds(LOW, 64 - LOW)

    load_q = pltpu.make_async_copy(queries, q, w_sem.at[16])
    load_q.start()
    weights = []
    for h in range(VIT_HEADS):
        copy = pltpu.make_async_copy(
            wo.at[pl.ds(h * VIT_HDIM, VIT_HDIM)], wov.at[h, pl.ds(0, VIT_HDIM)], w_sem.at[h]
        )
        copy.start()
        weights.append(copy)

    def own_part():
        column = lax.broadcasted_iota(jnp.int32, (64, PACKED), 1)
        rest = jnp.where(column == ONE_AT, 1.0, 0.0)
        rest = jnp.where((column == MASK_AT) & ~live, MASKED, rest)
        for h in range(VIT_HEADS):
            start = min(h * VIT_HDIM // HD * HD, VIT_D - PACKED)
            row = rest
            for which, at in ((2, 0), (1, KEY_AT), (0, QUERY_AT)):
                window = qkv[which, :, start : start + PACKED].astype(F32)
                shift = (at - (h * VIT_HDIM - start)) % PACKED
                if shift:
                    window = pltpu.roll(window, shift, 1)
                row = jnp.where((column >= at) & (column < at + VIT_HDIM), window, row)
            packed[h] = row.astype(BF16)
        kv[y, me] = packed[me]
        mw[x, zl] = merger[...]
        kw0[y, x, zl] = kvw[0:LOW]
        kw1[x, y, zl] = kvw[LOW:64]
        for h in range(VIT_HEADS):
            wov[h, VIT_HDIM:, :] = jnp.zeros((HD - VIT_HDIM, VIT_D), BF16)

    meet(peers, own_part)

    numbers, sends = {}, []

    def number(name):
        return numbers.setdefault(name, len(numbers))

    def go(name, src, dst, **device):
        k = number(name)
        copy = remote(src, dst, sent.at[k], got.at[k], **device)
        copy.start()
        sends.append(copy)

    def arrived(name, ref):
        k = number(name)
        remote(ref, ref, sent.at[k], got.at[k], y=up).wait_recv()

    lm_scale = HD**-0.5 * LOG2E
    lm_tiles = queries.shape[0] // 256

    def lm_rows(i):
        return pl.ds(i * 256, 256)

    def near_part():
        def near_score(i):
            extent = (i // 4 + 1) * 128
            keys = span[0, 0:extent, :]
            scores = nt_dot(q[lm_rows(i), :], keys)
            row = lax.broadcasted_iota(jnp.int32, (256, 128), 0)
            place_ = lax.broadcasted_iota(jnp.int32, (256, 128), 1)
            edge = jnp.where(
                place_ + (extent - 128) <= (i * 256 + row) // 8, scores[:, extent - 128 :], MASKED
            )
            if extent > 128:
                edge = jnp.concatenate([scores[:, : extent - 128], edge], axis=1)
            return edge, jnp.max(edge, axis=1, keepdims=True), extent

        ready = near_score(0)
        for i in range(lm_tiles):
            following = near_score(i + 1) if i + 1 < lm_tiles else None
            scores, top, extent = ready
            weights = jnp.exp2((scores - top) * lm_scale).astype(BF16)
            values = jnp.concatenate([span[1, 0:extent, :], jnp.ones((extent, HD), BF16)], axis=1)
            lacc[lm_rows(i), :] = jnp.dot(weights, values, preferred_element_type=F32)
            lpeak[lm_rows(i), :] = jnp.broadcast_to(top, (256, HD))
            ready = following

    def far_part(slots, store, between):
        keys = jnp.concatenate([vis[a, b, 0] for a, b in slots], axis=0)
        values = jnp.concatenate([vis[a, b, 1] for a, b in slots], axis=0)
        values = jnp.concatenate([values, jnp.ones((len(slots) * 128, HD), BF16)], axis=1)
        lane = lax.broadcasted_iota(jnp.int32, (1, HD), 1)

        def slot_bias(a, b):
            patch = ((b * 4 + (lane >> 4 & 3)) * 8 + a * 2 + (lane >> 6)) * 64 + (lane & 15) * 4
            return jnp.where(patch < total_patches, 0.0, MASKED)

        shift = jnp.concatenate([slot_bias(a, b) for a, b in slots], axis=1)

        def far_score(i):
            scores = nt_dot(q[lm_rows(i), :], keys) + shift
            old = lpeak[lm_rows(i), :]
            return scores, jnp.maximum(old, jnp.max(scores, axis=1, keepdims=True)), old

        ready = far_score(0)
        for i in range(lm_tiles):
            following = far_score(i + 1) if i + 1 < lm_tiles else None
            scores, top, old = ready
            spread = jnp.concatenate([top] * len(slots), axis=1)
            weights = jnp.exp2((scores - spread) * lm_scale).astype(BF16)
            total = jnp.dot(weights, values, preferred_element_type=F32)
            fade = jnp.exp2((old - top) * lm_scale)
            total += lacc[lm_rows(i), :] * jnp.concatenate([fade, fade], axis=1)
            store(i, total, top)
            between(i)
            ready = following

    for dz in RING_ORDER:
        for dc in range(2):
            if (dz, dc) != (0, 0):
                oz, oc_ = place(dz, dc)
                go(("a", dz, dc), packed.at[oz * 2 + oc_], kv.at[y, me], **device_of(oz, oc_))
    go(("k0", "e", 0), kvw.at[low], kw0.at[y, x, zl], x=east)
    go(("k0", "w", 0), kvw.at[low], kw0.at[y, x, zl], x=west)
    go(("w", "e", 0), merger, mw.at[x, zl], x=east)
    go(("w", "w", 0), merger, mw.at[x, zl], x=west)
    def blocks_of(row, dz):
        return kv.at[row, pl.ds(mod(z + 8 - dz, 8) * 2, 2)]

    def source_of(dz, dc):
        return mod(z + 8 - dz, 8) * 2 + mod(c + dc, 2)

    for i, dz in enumerate(RING_ORDER):
        for dc in range(2):
            if (dz, dc) != (0, 0):
                arrived(("a", dz, dc), kv.at[y, source_of(dz, dc)])
        blocks = blocks_of(y, dz)
        go(("y1", 0, i), blocks, blocks, y=up)
        go(("y1", 1, i), blocks, blocks, y=down)

    go(("k0", "z"), kvw.at[low], kw0.at[y, x, zl], zl=ozl)
    go(("k1", "z"), kvw.at[high], kw1.at[x, y, zl], zl=ozl)
    go(("w", "z"), merger, mw.at[x, zl], zl=ozl)
    row = lax.broadcasted_iota(jnp.int32, (PACKED, PACKED), 0)
    col = lax.broadcasted_iota(jnp.int32, (PACKED, PACKED), 1)
    moved = (col >= KEY_AT) & (col < QUERY_AT) & (row == col + (QUERY_AT - KEY_AT))
    pick = moved | ((col == MASK_AT) & (row == ONE_AT))
    pick = jnp.where(pick, 1.0, 0.0).astype(BF16)
    scale = VIT_HDIM**-0.5 * LOG2E

    def rows_of(tile):
        return pl.ds(tile * 256 if isinstance(tile, int) else pl.multiple_of(tile * 256, 256), 256)

    def score(tile, block, first):
        rows = rows_of(tile)
        scores = nt_dot(qp[rows, :], block)
        top = jnp.broadcast_to(jnp.max(scores, axis=1, keepdims=True), (256, HD))
        if first:
            return scores, top, None
        old = peak[rows, :]
        return scores, jnp.maximum(old, top), old

    def blend(tile, block, scores, top, old):
        rows = rows_of(tile)
        weights = jnp.exp2((scores - jnp.concatenate([top] * 8, axis=1)) * scale)
        total = jnp.dot(weights.astype(BF16), block, preferred_element_type=F32)
        if old is not None:
            fade = jnp.exp2((old - top) * scale)
            total += acc[rows, :] * jnp.concatenate([fade, fade], axis=1)
        peak[rows, :] = top
        return total

    def whole(slot, first, tiles=(0, 1, 2, 3), store=None):
        block = kv[slot].reshape(1024, PACKED)
        ready = score(tiles[0], block, first)
        for t, tile in enumerate(tiles):
            following = score(tiles[t + 1], block, first) if t < 3 else None
            total = blend(tile, block, *ready)
            if store is None:
                acc[rows_of(tile), :] = total
            else:
                store(t, tile, total)
            ready = following

    qp[...] = jnp.dot(
        kv[y].reshape(1024, PACKED), pick, preferred_element_type=F32
    ).astype(BF16)
    whole(y, True)

    for i, dz in enumerate(RING_ORDER):
        way, origin, target = ((0, down, up), (1, up, down))[i % 2]
        blocks = blocks_of(origin, dz)
        arrived(("y1", way, i), blocks)
        go(("y2", i), blocks, blocks, y=target)
    arrived(("k0", "z"), kw0.at[y, x, ozl])
    go(("k0", "e", 1), kw0.at[y, x, ozl], kw0.at[y, x, ozl], x=east)
    go(("k0", "w", 1), kw0.at[y, x, ozl], kw0.at[y, x, ozl], x=west)
    arrived(("k1", "z"), kw1.at[x, y, ozl])

    def piece(row, k):
        block = kw1.at[x, row]
        go(("k1", "e", k), block, block, x=east)
        go(("k1", "w", k), block, block, x=west)

    piece(y, 0)

    go(("k1", "u"), kw1.at[x, y], kw1.at[x, y], y=up)
    go(("k1", "d"), kw1.at[x, y], kw1.at[x, y], y=down)
    for i, dz in enumerate(RING_ORDER):
        way, origin = ((1, up), (0, down))[i % 2]
        arrived(("y1", way, i), blocks_of(origin, dz))

    whole(down, False)
    arrived(("k0", "e", 0), kw0.at[y, west, zl])
    go(("k0", "e", 2), kw0.at[y, west, zl], kw0.at[y, west, zl], x=east)
    arrived(("w", "e", 0), mw.at[west, zl])
    go(("w", "e", 2), mw.at[west, zl], mw.at[west, zl], x=east)
    whole(up, False)
    arrived(("k0", "w", 1), kw0.at[y, east, ozl])
    go(("k0", "w", 2), kw0.at[y, east, ozl], kw0.at[y, east, ozl], x=west)
    for i, dz in enumerate(RING_ORDER):
        arrived(("y2", i), blocks_of(across, dz))

    def give_back(t, tile, total):
        done = (total[:, :HD] / total[:, ONE_AT : ONE_AT + 1]).astype(BF16)
        back[pl.ds(tile * 4, 4)] = done.reshape(4, 64, HD)
        for dzl in range(2):
            for dc in range(2):
                if (t, dzl, dc) == (3, 0, 0):
                    continue
                tzl, tc = mod(zl + dzl, 2), mod(c + dc, 2)
                go(
                    ("o", t, dzl, dc), back.at[tile * 4 + tzl * 2 + tc], att.at[me],
                    zh=tile, zl=tzl, c=tc,
                )

    turns = (2, 1, 3, 0)
    whole(across, False, [mod(zh + turn, 4) for turn in turns], give_back)
    att[me] = back[me]

    arrived(("w", "z"), mw.at[x, ozl])
    go(("w", "e", 1), mw.at[x, ozl], mw.at[x, ozl], x=east)
    go(("w", "w", 1), mw.at[x, ozl], mw.at[x, ozl], x=west)
    for copy in weights:
        copy.wait()
    for t in range(4):
        for dzl in range(2):
            for dc in range(2):
                if (t, dzl, dc) != (3, 0, 0):
                    source = mod(zh + 4 - turns[t], 4) * 4 + mod(zl + dzl, 2) * 2 + mod(c + dc, 2)
                    arrived(("o", t, dzl, dc), att.at[source])

    hidden = jnp.zeros((64, VIT_D), F32)
    for h in range(0, VIT_HEADS, 2):
        both = jnp.concatenate([att[h], att[h + 1]], axis=1)
        hidden += jnp.dot(
            both, wov[pl.ds(h, 2)].reshape(2 * HD, VIT_D), preferred_element_type=F32
        )
    hidden = jnp.where(live[:, :1], hidden, 0.0)
    centred = hidden - jnp.mean(hidden, axis=1, keepdims=True)
    spread = jnp.mean(centred * centred, axis=1, keepdims=True)
    normed = (centred * lax.rsqrt(spread + 1e-6) * gain[...][None, :]).astype(BF16).astype(F32)
    for i in range(VIT_D // HD):
        nf[pl.ds(i * 64, 64), :] = normed[:, i * HD : (i + 1) * HD]

    lane = lax.broadcasted_iota(jnp.int32, (16, VIT_D), 1)
    quarter = [
        jnp.concatenate(
            [nf[pl.ds(i * 64 + j, 16, stride=4), :] for i in range(VIT_D // HD)], axis=1
        )
        for j in range(4)
    ]
    for part in range(4):
        laid = jnp.zeros((16, VIT_D), F32)
        for j in range(4):
            for half in range(2):
                start = 320 * j + 160 * half
                origin = 640 * half + 160 * part
                shift = (start - origin) % VIT_D
                rolled = pltpu.roll(quarter[j], shift, 1) if shift else quarter[j]
                laid = jnp.where((lane >= start) & (lane < start + 160), rolled, laid)
        slab[part] = laid.astype(BF16)
    for dy in range(1, 4):
        oy = mod(y + dy, 4)
        go(("m", dy), slab.at[oy], mid.at[y], y=oy)
    mid[y] = slab[y]

    arrived(("w", "w", 1), mw.at[east, ozl])
    go(("w", "w", 2), mw.at[east, ozl], mw.at[east, ozl], x=west)
    arrived(("k1", "u"), kw1.at[x, down])
    go(("k1", "u", 2), kw1.at[x, down, 0], kw1.at[x, down, 0], y=up)
    piece(down, 1)
    arrived(("k1", "d"), kw1.at[x, up])
    go(("k1", "d", 2), kw1.at[x, up, 1], kw1.at[x, up, 1], y=down)
    piece(up, 2)
    arrived(("k0", "w", 0), kw0.at[y, east, zl])
    arrived(("k0", "e", 1), kw0.at[y, west, ozl])
    arrived(("k0", "e", 2), kw0.at[y, xfar, zl])
    arrived(("k0", "w", 2), kw0.at[y, xfar, ozl])
    go(("k0", "u"), kw0.at[y], kw0.at[y], y=up)
    go(("k0", "d"), kw0.at[y], kw0.at[y], y=down)
    for dy in range(1, 4):
        arrived(("m", dy), mid.at[mod(y + 4 - dy, 4)])

    mine = zh * 2 + c
    head, tail = pl.ds(0, 2), pl.ds(2, 2)
    go("t0", mid.at[head], tok.at[mine, head], zh=right)
    go("t1", mid.at[tail], tok.at[mine, tail], zh=left)
    go("t2", mid, tok.at[mine], c=oc)
    go("t9", mid.at[tail], tok.at[mine, tail], zh=right)
    go("t10", mid.at[head], tok.at[mine, head], zh=left)
    tok[mine] = mid[...]
    load_q.wait()
    near_part()
    arrived(("k1", "u", 2), kw1.at[x, across, 0])
    arrived(("k1", "d", 2), kw1.at[x, across, 1])
    piece(across, 3)

    def piece_on(k, row):
        if k < 2:
            block, way, target = kw1.at[west, row], "e", east
        else:
            block, way, target = kw1.at[east, row], "w", west
        arrived(("k1", way, k), block)
        go(("k1", way, k, 2), block, block, x=target)

    piece_on(0, y)
    here, there = tok.at[left * 2 + c], tok.at[right * 2 + c]
    arrived("t0", here.at[head])
    go("t3", here.at[head], here.at[head], zh=right)
    arrived("t1", there.at[tail])
    go("t5", there.at[tail], there.at[tail], zh=left)
    arrived("t9", here.at[tail])
    go("t4", here, here, c=oc)
    arrived("t10", there.at[head])
    go("t6", there, there, c=oc)
    first, second = (tok.at[far * 2 + c].at[pl.ds(i, 2)] for i in (0, 2))
    arrived("t3", first)
    go("t7", first, first, c=oc)
    arrived("t5", second)
    go("t8", second, second, c=oc)
    piece_on(1, down)
    piece_on(2, up)
    arrived(("k0", "u"), kw0.at[down])
    go(("k0", "u", 2), kw0.at[down, pl.ds(0, 2)], kw0.at[down, pl.ds(0, 2)], y=up)
    arrived(("k0", "d"), kw0.at[up])
    go(("k0", "d", 2), kw0.at[up, pl.ds(2, 2)], kw0.at[up, pl.ds(2, 2)], y=down)
    arrived("t2", tok.at[zh * 2 + oc])
    arrived("t4", tok.at[left * 2 + oc])
    arrived("t6", tok.at[right * 2 + oc])
    arrived("t7", tok.at[far * 2 + oc].at[pl.ds(0, 2)])
    arrived("t8", tok.at[far * 2 + oc].at[pl.ds(2, 2)])
    arrived(("w", "w", 0), mw.at[east, zl])
    arrived(("w", "e", 1), mw.at[west, ozl])
    arrived(("w", "e", 2), mw.at[xfar, zl])
    arrived(("w", "w", 2), mw.at[xfar, ozl])

    def part(index):
        rows = tok[pl.ds(index * 2, 2)].reshape(128, VIT_D)
        return jnp.dot(rows, mw[...].reshape(VIT_D, 1024), preferred_element_type=F32)

    sb[0] = part(across).astype(BF16)
    go("s0", sb.at[0, pl.ds(0, 64)], ra.at[0], y=up)
    go("s1", sb.at[0, pl.ds(64, 64)], ra.at[1], y=down)
    nxt, prv = part(up), part(down)
    sb[1, 64:128] = nxt[64:128].astype(BF16)
    sb[2, 0:64] = prv[0:64].astype(BF16)
    go("s2", sb.at[1, pl.ds(64, 64)], rb.at[0, pl.ds(64, 64)], y=up)
    go("s3", sb.at[2, pl.ds(0, 64)], rb.at[1, pl.ds(0, 64)], y=down)
    arrived("s0", ra.at[0])
    sb[1, 0:64] = (nxt[0:64] + ra[0].astype(F32)).astype(BF16)
    go("s4", sb.at[1, pl.ds(0, 64)], rb.at[0, pl.ds(0, 64)], y=up)
    arrived("s1", ra.at[1])
    sb[2, 64:128] = (prv[64:128] + ra[1].astype(F32)).astype(BF16)
    go("s5", sb.at[2, pl.ds(64, 64)], rb.at[1, pl.ds(64, 64)], y=down)
    own = part(y)
    piece_on(3, across)
    arrived("s2", rb.at[0, pl.ds(64, 64)])
    arrived("s3", rb.at[1, pl.ds(0, 64)])
    arrived("s4", rb.at[0, pl.ds(0, 64)])
    arrived("s5", rb.at[1, pl.ds(64, 64)])
    embedded = (own + rb[0].astype(F32) + rb[1].astype(F32)).astype(BF16).astype(F32)
    square = jnp.sum(embedded * embedded, axis=1, keepdims=True)
    turned = jnp.transpose(jnp.broadcast_to(square, (128, 128)))
    others = [(dzh, dc) for dzh in range(4) for dc in range(2) if dzh or dc]
    ssr[zh * 2 + c] = turned[0:8]
    for dzh, dc in others:
        slot = ssr.at[zh * 2 + c]
        go(("q", dzh, dc), slot, slot, zh=mod(zh + dzh, 4), c=mod(c + dc, 2))
    scaled = (embedded * lm_gain[...][None, :]).astype(BF16)
    arrived(("k0", "u", 2), kw0.at[across, pl.ds(0, 2)])
    arrived(("k0", "d", 2), kw0.at[across, pl.ds(2, 2)])
    for k, row in enumerate((y, down, up, across)):
        if k < 2:
            arrived(("k1", "w", k), kw1.at[east, row])
            arrived(("k1", "e", k, 2), kw1.at[xfar, row])
        else:
            arrived(("k1", "e", k), kw1.at[west, row])
            arrived(("k1", "w", k, 2), kw1.at[xfar, row])

    def head_rows(k, t):
        kx, kz = 2 * k + t // 4, t % 4 // 2
        pieces = []
        for e in range(2):
            ky = 2 * (t % 2) + e
            pieces += [kw0[ky, kx, kz], kw1[kx, ky, kz]]
        return pieces

    for k in range(2):
        for t in range(0, 8, 2):
            both = jnp.concatenate(head_rows(k, t) + head_rows(k, t + 1), axis=0)
            both = nt_dot(scaled, both)
            kvf[k * 8 + t] = both[:, :128]
            kvf[k * 8 + t + 1] = both[:, 128:]

    for j in range(4):
        for k in range(2):
            cs[j, k] = kvf[k * 8 + j * 2 + oc].astype(BF16)
    go("c", cs, cr, c=oc)
    arrived("c", cr)

    def term(j, k):
        return kvf[k * 8 + j * 2 + c] + cr[j, k].astype(F32)

    for k in range(2):
        ks[0, k] = term(far, k).astype(BF16)
    go("z0", ks.at[0, 0], ka.at[0], zh=right)
    go("z1", ks.at[0, 1], ka.at[1], zh=left)
    ks[1, 1] = term(right, 1).astype(BF16)
    ks[2, 0] = term(left, 0).astype(BF16)
    go("z2", ks.at[1, 1], kb.at[0, 1], zh=right)
    go("z3", ks.at[2, 0], kb.at[1, 0], zh=left)
    arrived("z0", ka.at[0])
    ks[1, 0] = (term(right, 0) + ka[0].astype(F32)).astype(BF16)
    go("z4", ks.at[1, 0], kb.at[0, 0], zh=right)
    arrived("z1", ka.at[1])
    ks[2, 1] = (term(left, 1) + ka[1].astype(F32)).astype(BF16)
    go("z5", ks.at[2, 1], kb.at[1, 1], zh=left)
    for dzh, dc in others:
        arrived(("q", dzh, dc), ssr.at[mod(zh + 4 - dzh, 4) * 2 + mod(c + dc, 2)])
    total = jnp.sum(ssr[...], axis=0)[0:1]
    factor = lax.rsqrt(jnp.broadcast_to(total, (128, 128)) / D + 1e-6)
    factor = jnp.transpose(factor)
    arrived("z2", kb.at[0, 1])
    arrived("z3", kb.at[1, 0])
    arrived("z4", kb.at[0, 0])
    arrived("z5", kb.at[1, 1])
    for k in range(2):
        done = term(zh, k) + kb[0, k].astype(F32) + kb[1, k].astype(F32)
        vis[y, zl, k] = (done * factor).astype(BF16)

    first = vis.at[y, zl]
    go("v0", first, first, zl=ozl)
    go("v1", first, first, y=up)
    go("v2", first, first, y=down)
    second = vis.at[y, ozl]
    arrived("v0", second)
    go("v3", second, second, y=up)
    go("v4", second, second, y=down)
    below = vis.at[down, zl]
    arrived("v1", below)
    go("v5", below, below, y=up)
    arrived("v2", vis.at[up, zl])

    def keep(i, total, top):
        lacc[lm_rows(i), :] = total
        lpeak[lm_rows(i), :] = top

    def pass_up(i):
        if i == 3:
            above = vis.at[up, ozl]
            arrived("v4", above)
            go("v6", above, above, y=down)

    far_part([(y, zl), (y, ozl), (down, zl), (up, zl)], keep, pass_up)
    arrived("v3", vis.at[down, ozl])
    arrived("v5", vis.at[across, zl])
    arrived("v6", vis.at[across, ozl])
    stores = []

    def finish(i, total, top):
        result[lm_rows(i), :] = (total[:, :HD] / total[:, HD:]).astype(BF16)

    def write(i):
        if i % 4 == 3:
            rows = pl.ds((i - 3) * 256, 1024)
            copy = pltpu.make_async_copy(result.at[rows], out.at[rows], w_sem.at[17 + i // 4])
            copy.start()
            stores.append(copy)

    far_part([(down, ozl), (up, ozl), (across, zl), (across, ozl)], finish, write)
    assert len(numbers) == COPIES, len(numbers)
    for copy in sends:
        copy.wait_send()
    for copy in stores:
        copy.wait()


def attend(counts, qkv, wo, gain, merger, kvw, lm_gain, queries, span):
    dma = pltpu.SemaphoreType.DMA
    vmem = pl.BlockSpec(memory_space=pltpu.VMEM)
    hbm = pl.BlockSpec(memory_space=pl.ANY)
    return pl.pallas_call(
        front_kernel,
        out_shape=jax.ShapeDtypeStruct(queries.shape, BF16),
        in_specs=[
            pl.BlockSpec(memory_space=pltpu.SMEM), vmem, hbm, vmem, vmem, vmem, vmem, hbm, vmem,
        ],
        out_specs=hbm,
        scratch_shapes=[
            pltpu.VMEM((16, 64, PACKED), BF16),
            pltpu.VMEM((4, 16, 64, PACKED), BF16),
            pltpu.VMEM((1024, PACKED), BF16),
            pltpu.VMEM((1024, PACKED), F32),
            pltpu.VMEM((1024, HD), F32),
            pltpu.VMEM((16, 64, HD), BF16),
            pltpu.VMEM((16, 64, HD), BF16),
            pltpu.VMEM((16, HD, VIT_D), BF16),
            pltpu.VMEM((64 * VIT_D // HD, HD), F32),
            pltpu.VMEM((4, 16, VIT_D), BF16),
            pltpu.VMEM((4, 16, VIT_D), BF16),
            pltpu.VMEM((8, 4, 16, VIT_D), BF16),
            pltpu.VMEM((4, 2, 160, 1024), BF16),
            pltpu.VMEM((4, 4, 2, LOW, 1024), BF16),
            pltpu.VMEM((4, 4, 2, 64 - LOW, 1024), BF16),
            pltpu.VMEM((3, 128, 1024), BF16),
            pltpu.VMEM((2, 64, 1024), BF16),
            pltpu.VMEM((2, 128, 1024), BF16),
            pltpu.VMEM((16, 128, 128), F32),
            pltpu.VMEM((4, 2, 128, 128), BF16),
            pltpu.VMEM((4, 2, 128, 128), BF16),
            pltpu.VMEM((3, 2, 128, 128), BF16),
            pltpu.VMEM((2, 128, 128), BF16),
            pltpu.VMEM((2, 2, 128, 128), BF16),
            pltpu.VMEM((8, 8, 128), F32),
            pltpu.VMEM((4, 2, 2, 128, 128), BF16),
            pltpu.VMEM((4096, HD), BF16),
            pltpu.VMEM((4096, 2 * HD), F32),
            pltpu.VMEM((4096, HD), F32),
            pltpu.VMEM((4096, HD), BF16),
            dma((21,)), dma((COPIES,)), dma((COPIES,)),
        ],
        compiler_params=pltpu.CompilerParams(
            collective_id=0, has_side_effects=True, vmem_limit_bytes=61 * 2**20
        ),
        cost_estimate=pl.CostEstimate(
            flops=60_000_000_000, bytes_accessed=8_000_000, transcendentals=4_200_000
        ),
        name="front",
    )(counts, qkv, wo, gain, merger, kvw, lm_gain, queries, span)


def local(
    vit_qkv,
    patch_counts,
    vit_out_weight,
    vit_norm_gain,
    merger_weight,
    lm_norm_gain,
    kv_weight,
    queries,
    span_kv,
):
    rows = queries.shape[1] * queries.shape[2]
    span = span_kv[0, :, :, 0].transpose(1, 0, 2)
    out = attend(
        patch_counts, vit_qkv[0].transpose(1, 0, 2), vit_out_weight, vit_norm_gain,
        merger_weight, kv_weight.T, lm_norm_gain, queries.reshape(rows, HD), span,
    )
    return out.reshape(queries.shape)


def solution(mesh):
    fine = Mesh(mesh.devices.reshape(4, 2, 4, 4, 2), ("x", "zl", "y", "zh", "c"))
    placed = (
        P("x", (*SEQ, *TP), None, None),
        P("x"),
        P(),
        P(),
        P(IMG_SEQ, TP),
        P(TP),
        P(TP, IMG_SEQ),
        P("x", SEQ, TP, None),
        P("x", SEQ, None, TP, None),
    )
    return jax.shard_map(
        local, mesh=fine, in_specs=placed, out_specs=P("x", SEQ, TP, None), check_vma=False
    )
```

```python
import jax
import jax.numpy as jnp
from jax import lax
from jax.experimental import pallas as pl
from jax.experimental.pallas import tpu as pltpu
from jax.sharding import Mesh
from jax.sharding import PartitionSpec as P

VIT_D = 1280
VIT_HEADS = 16
VIT_HDIM = 80
D = 8192
HQ = 64
KVH = 8
HD = 128
SEQ = ("zl", "y")
TP = ("zh", "c")
IMG_SEQ = ("x", "zl", "y")
MASKED = -1e30
LOG2E = 1.4426950408889634
F32 = jnp.float32
BF16 = jnp.bfloat16

LOW = 16
COPIES = 130
ONE_AT, MASK_AT, KEY_AT, QUERY_AT, PACKED = 80, 81, 82, 162, 256
RING_ORDER = (0, 1, 7, 2, 6, 3, 5, 4)


def remote(src, dst, send_sem, recv_sem, **device):
    return pltpu.make_async_remote_copy(
        src_ref=src,
        dst_ref=dst,
        send_sem=send_sem,
        recv_sem=recv_sem,
        device_id=device,
        device_id_type=pl.DeviceIdType.MESH,
    )


def mod(a, n):
    return lax.rem(a, n)


def meet(peers, meanwhile):
    barrier = pltpu.get_barrier_semaphore()
    for device in peers:
        pl.semaphore_signal(
            barrier, inc=1, device_id=device, device_id_type=pl.DeviceIdType.MESH
        )
    meanwhile()
    pl.semaphore_wait(barrier, len(peers))


def nt_dot(a, b):
    return lax.dot_general(a, b, (((1,), (1,)), ((), ())), preferred_element_type=F32)


def front_kernel(
    counts, qkv, wo, gain, merger, kvw, lm_gain, queries, span, out,
    packed, kv, qp, acc, peak, back, att, wov, nf, slab, mid, tok,
    mw, kw0, kw1, sb, ra, rb, kvf, cs, cr, ks, ka, kb, ssr, vis, q, lacc, lpeak, result,
    w_sem, sent, got,
):
    x, y, zh, zl, c = (lax.axis_index(a) for a in ("x", "y", "zh", "zl", "c"))
    z = zh * 2 + zl
    me = z * 2 + c
    up, down, across = mod(y + 1, 4), mod(y + 3, 4), mod(y + 2, 4)
    right, left, far = mod(zh + 1, 4), mod(zh + 3, 4), mod(zh + 2, 4)
    east, west, xfar = mod(x + 1, 4), mod(x + 3, 4), mod(x + 2, 4)
    oc, ozl = 1 - c, 1 - zl

    def place(dz, dc):
        other = mod(z + dz, 8)
        return other, mod(c + dc, 2)

    def device_of(other_z, other_c):
        return {"zh": lax.div(other_z, 2), "zl": mod(other_z, 2), "c": other_c}

    order = [(dz, dc) for dz in RING_ORDER for dc in range(2)]
    peers = [device_of(*place(dz, dc)) for dz, dc in order if (dz, dc) != (0, 0)]
    peers += [{"y": up}, {"y": down}, {"y": across}, {"x": east}, {"x": west}]
    total_patches = counts[0]
    first_patch = ((zl * 4 + y) * 8 + zh * 2 + c) * 64
    live = first_patch + lax.broadcasted_iota(jnp.int32, (64, PACKED), 0) < total_patches
    low, high = pl.ds(0, LOW), pl.ds(LOW, 64 - LOW)

    load_q = pltpu.make_async_copy(queries, q, w_sem.at[16])
    load_q.start()
    weights = []
    for h in range(VIT_HEADS):
        copy = pltpu.make_async_copy(
            wo.at[pl.ds(h * VIT_HDIM, VIT_HDIM)], wov.at[h, pl.ds(0, VIT_HDIM)], w_sem.at[h]
        )
        copy.start()
        weights.append(copy)

    def own_part():
        column = lax.broadcasted_iota(jnp.int32, (64, PACKED), 1)
        rest = jnp.where(column == ONE_AT, 1.0, 0.0)
        rest = jnp.where((column == MASK_AT) & ~live, MASKED, rest)
        for h in range(VIT_HEADS):
            start = min(h * VIT_HDIM // HD * HD, VIT_D - PACKED)
            row = rest
            for which, at in ((2, 0), (1, KEY_AT), (0, QUERY_AT)):
                window = qkv[which, :, start : start + PACKED].astype(F32)
                shift = (at - (h * VIT_HDIM - start)) % PACKED
                if shift:
                    window = pltpu.roll(window, shift, 1)
                row = jnp.where((column >= at) & (column < at + VIT_HDIM), window, row)
            packed[h] = row.astype(BF16)
        kv[y, me] = packed[me]
        mw[x, zl] = merger[...]
        kw0[y, x, zl] = kvw[0:LOW]
        kw1[x, y, zl] = kvw[LOW:64]
        for h in range(VIT_HEADS):
            wov[h, VIT_HDIM:, :] = jnp.zeros((HD - VIT_HDIM, VIT_D), BF16)

    meet(peers, own_part)

    numbers, sends = {}, []

    def number(name):
        return numbers.setdefault(name, len(numbers))

    def go(name, src, dst, **device):
        k = number(name)
        copy = remote(src, dst, sent.at[k], got.at[k], **device)
        copy.start()
        sends.append(copy)

    def arrived(name, ref):
        k = number(name)
        remote(ref, ref, sent.at[k], got.at[k], y=up).wait_recv()

    lm_scale = HD**-0.5 * LOG2E
    lm_tiles = queries.shape[0] // 256

    def lm_rows(i):
        return pl.ds(i * 256, 256)

    def near_part():
        def near_score(i):
            extent = (i // 4 + 1) * 128
            keys = span[0, 0:extent, :]
            scores = nt_dot(q[lm_rows(i), :], keys)
            row = lax.broadcasted_iota(jnp.int32, (256, 128), 0)
            place_ = lax.broadcasted_iota(jnp.int32, (256, 128), 1)
            edge = jnp.where(
                place_ + (extent - 128) <= (i * 256 + row) // 8, scores[:, extent - 128 :], MASKED
            )
            if extent > 128:
                edge = jnp.concatenate([scores[:, : extent - 128], edge], axis=1)
            return edge, jnp.max(edge, axis=1, keepdims=True), extent

        ready = near_score(0)
        for i in range(lm_tiles):
            following = near_score(i + 1) if i + 1 < lm_tiles else None
            scores, top, extent = ready
            weights = jnp.exp2((scores - top) * lm_scale).astype(BF16)
            values = jnp.concatenate([span[1, 0:extent, :], jnp.ones((extent, HD), BF16)], axis=1)
            lacc[lm_rows(i), :] = jnp.dot(weights, values, preferred_element_type=F32)
            lpeak[lm_rows(i), :] = jnp.broadcast_to(top, (256, HD))
            ready = following

    def far_part(slots, store, between):
        keys = jnp.concatenate([vis[a, b, 0] for a, b in slots], axis=0)
        values = jnp.concatenate([vis[a, b, 1] for a, b in slots], axis=0)
        values = jnp.concatenate([values, jnp.ones((len(slots) * 128, HD), BF16)], axis=1)
        lane = lax.broadcasted_iota(jnp.int32, (1, HD), 1)

        def slot_bias(a, b):
            patch = ((b * 4 + (lane >> 4 & 3)) * 8 + a * 2 + (lane >> 6)) * 64 + (lane & 15) * 4
            return jnp.where(patch < total_patches, 0.0, MASKED)

        shift = jnp.concatenate([slot_bias(a, b) for a, b in slots], axis=1)

        def far_score(i):
            scores = nt_dot(q[lm_rows(i), :], keys) + shift
            old = lpeak[lm_rows(i), :]
            return scores, jnp.maximum(old, jnp.max(scores, axis=1, keepdims=True)), old

        ready = far_score(0)
        for i in range(lm_tiles):
            following = far_score(i + 1) if i + 1 < lm_tiles else None
            scores, top, old = ready
            spread = jnp.concatenate([top] * len(slots), axis=1)
            weights = jnp.exp2((scores - spread) * lm_scale).astype(BF16)
            total = jnp.dot(weights, values, preferred_element_type=F32)
            fade = jnp.exp2((old - top) * lm_scale)
            total += lacc[lm_rows(i), :] * jnp.concatenate([fade, fade], axis=1)
            store(i, total, top)
            between(i)
            ready = following

    for dz in RING_ORDER:
        for dc in range(2):
            if (dz, dc) != (0, 0):
                oz, oc_ = place(dz, dc)
                go(("a", dz, dc), packed.at[oz * 2 + oc_], kv.at[y, me], **device_of(oz, oc_))
    go(("k0", "e", 0), kvw.at[low], kw0.at[y, x, zl], x=east)
    go(("k0", "w", 0), kvw.at[low], kw0.at[y, x, zl], x=west)
    go(("w", "e", 0), merger, mw.at[x, zl], x=east)
    go(("w", "w", 0), merger, mw.at[x, zl], x=west)
    def blocks_of(row, dz):
        return kv.at[row, pl.ds(mod(z + 8 - dz, 8) * 2, 2)]

    def source_of(dz, dc):
        return mod(z + 8 - dz, 8) * 2 + mod(c + dc, 2)

    for i, dz in enumerate(RING_ORDER):
        for dc in range(2):
            if (dz, dc) != (0, 0):
                arrived(("a", dz, dc), kv.at[y, source_of(dz, dc)])
        blocks = blocks_of(y, dz)
        go(("y1", 0, i), blocks, blocks, y=up)
        go(("y1", 1, i), blocks, blocks, y=down)

    go(("k0", "z"), kvw.at[low], kw0.at[y, x, zl], zl=ozl)
    go(("k1", "z"), kvw.at[high], kw1.at[x, y, zl], zl=ozl)
    go(("w", "z"), merger, mw.at[x, zl], zl=ozl)
    row = lax.broadcasted_iota(jnp.int32, (PACKED, PACKED), 0)
    col = lax.broadcasted_iota(jnp.int32, (PACKED, PACKED), 1)
    moved = (col >= KEY_AT) & (col < QUERY_AT) & (row == col + (QUERY_AT - KEY_AT))
    pick = moved | ((col == MASK_AT) & (row == ONE_AT))
    pick = jnp.where(pick, 1.0, 0.0).astype(BF16)
    scale = VIT_HDIM**-0.5 * LOG2E

    def rows_of(tile):
        return pl.ds(tile * 256 if isinstance(tile, int) else pl.multiple_of(tile * 256, 256), 256)

    def score(tile, block, first):
        rows = rows_of(tile)
        scores = nt_dot(qp[rows, :], block)
        top = jnp.broadcast_to(jnp.max(scores, axis=1, keepdims=True), (256, HD))
        if first:
            return scores, top, None
        old = peak[rows, :]
        return scores, jnp.maximum(old, top), old

    def blend(tile, block, scores, top, old):
        rows = rows_of(tile)
        weights = jnp.exp2((scores - jnp.concatenate([top] * 8, axis=1)) * scale)
        total = jnp.dot(weights.astype(BF16), block, preferred_element_type=F32)
        if old is not None:
            fade = jnp.exp2((old - top) * scale)
            total += acc[rows, :] * jnp.concatenate([fade, fade], axis=1)
        peak[rows, :] = top
        return total

    def whole(slot, first, tiles=(0, 1, 2, 3), store=None):
        block = kv[slot].reshape(1024, PACKED)
        ready = score(tiles[0], block, first)
        for t, tile in enumerate(tiles):
            following = score(tiles[t + 1], block, first) if t < 3 else None
            total = blend(tile, block, *ready)
            if store is None:
                acc[rows_of(tile), :] = total
            else:
                store(t, tile, total)
            ready = following

    qp[...] = jnp.dot(
        kv[y].reshape(1024, PACKED), pick, preferred_element_type=F32
    ).astype(BF16)
    whole(y, True)

    for i, dz in enumerate(RING_ORDER):
        way, origin, target = ((0, down, up), (1, up, down))[i % 2]
        blocks = blocks_of(origin, dz)
        arrived(("y1", way, i), blocks)
        go(("y2", i), blocks, blocks, y=target)
    arrived(("k0", "z"), kw0.at[y, x, ozl])
    go(("k0", "e", 1), kw0.at[y, x, ozl], kw0.at[y, x, ozl], x=east)
    go(("k0", "w", 1), kw0.at[y, x, ozl], kw0.at[y, x, ozl], x=west)
    arrived(("k1", "z"), kw1.at[x, y, ozl])

    def piece(row, k):
        block = kw1.at[x, row]
        go(("k1", "e", k), block, block, x=east)
        go(("k1", "w", k), block, block, x=west)

    piece(y, 0)

    go(("k1", "u"), kw1.at[x, y], kw1.at[x, y], y=up)
    go(("k1", "d"), kw1.at[x, y], kw1.at[x, y], y=down)
    for i, dz in enumerate(RING_ORDER):
        way, origin = ((1, up), (0, down))[i % 2]
        arrived(("y1", way, i), blocks_of(origin, dz))

    whole(down, False)
    arrived(("k0", "e", 0), kw0.at[y, west, zl])
    go(("k0", "e", 2), kw0.at[y, west, zl], kw0.at[y, west, zl], x=east)
    arrived(("w", "e", 0), mw.at[west, zl])
    go(("w", "e", 2), mw.at[west, zl], mw.at[west, zl], x=east)
    whole(up, False)
    arrived(("k0", "w", 1), kw0.at[y, east, ozl])
    go(("k0", "w", 2), kw0.at[y, east, ozl], kw0.at[y, east, ozl], x=west)
    for i, dz in enumerate(RING_ORDER):
        arrived(("y2", i), blocks_of(across, dz))

    def give_back(t, tile, total):
        done = (total[:, :HD] / total[:, ONE_AT : ONE_AT + 1]).astype(BF16)
        back[pl.ds(tile * 4, 4)] = done.reshape(4, 64, HD)
        for dzl in range(2):
            for dc in range(2):
                if (t, dzl, dc) == (3, 0, 0):
                    continue
                tzl, tc = mod(zl + dzl, 2), mod(c + dc, 2)
                go(
                    ("o", t, dzl, dc), back.at[tile * 4 + tzl * 2 + tc], att.at[me],
                    zh=tile, zl=tzl, c=tc,
                )

    turns = (2, 1, 3, 0)
    whole(across, False, [mod(zh + turn, 4) for turn in turns], give_back)
    att[me] = back[me]

    arrived(("w", "z"), mw.at[x, ozl])
    go(("w", "e", 1), mw.at[x, ozl], mw.at[x, ozl], x=east)
    go(("w", "w", 1), mw.at[x, ozl], mw.at[x, ozl], x=west)
    arrived(("k1", "u"), kw1.at[x, down])
    go(("k1", "u", 2), kw1.at[x, down, 0], kw1.at[x, down, 0], y=up)
    piece(down, 1)
    arrived(("k1", "d"), kw1.at[x, up])
    go(("k1", "d", 2), kw1.at[x, up, 1], kw1.at[x, up, 1], y=down)
    piece(up, 2)
    arrived(("k0", "w", 0), kw0.at[y, east, zl])
    arrived(("k0", "e", 1), kw0.at[y, west, ozl])
    arrived(("k0", "e", 2), kw0.at[y, xfar, zl])
    arrived(("k0", "w", 2), kw0.at[y, xfar, ozl])
    go(("k0", "u"), kw0.at[y], kw0.at[y], y=up)
    go(("k0", "d"), kw0.at[y], kw0.at[y], y=down)
    for copy in weights:
        copy.wait()
    for t in range(4):
        for dzl in range(2):
            for dc in range(2):
                if (t, dzl, dc) != (3, 0, 0):
                    source = mod(zh + 4 - turns[t], 4) * 4 + mod(zl + dzl, 2) * 2 + mod(c + dc, 2)
                    arrived(("o", t, dzl, dc), att.at[source])

    hidden = jnp.zeros((64, VIT_D), F32)
    for h in range(0, VIT_HEADS, 2):
        both = jnp.concatenate([att[h], att[h + 1]], axis=1)
        hidden += jnp.dot(
            both, wov[pl.ds(h, 2)].reshape(2 * HD, VIT_D), preferred_element_type=F32
        )
    hidden = jnp.where(live[:, :1], hidden, 0.0)
    centred = hidden - jnp.mean(hidden, axis=1, keepdims=True)
    spread = jnp.mean(centred * centred, axis=1, keepdims=True)
    normed = (centred * lax.rsqrt(spread + 1e-6) * gain[...][None, :]).astype(BF16).astype(F32)
    for i in range(VIT_D // HD):
        nf[pl.ds(i * 64, 64), :] = normed[:, i * HD : (i + 1) * HD]

    lane = lax.broadcasted_iota(jnp.int32, (16, VIT_D), 1)
    quarter = [
        jnp.concatenate(
            [nf[pl.ds(i * 64 + j, 16, stride=4), :] for i in range(VIT_D // HD)], axis=1
        )
        for j in range(4)
    ]
    for part in range(4):
        laid = jnp.zeros((16, VIT_D), F32)
        for j in range(4):
            for half in range(2):
                start = 320 * j + 160 * half
                origin = 640 * half + 160 * part
                shift = (start - origin) % VIT_D
                rolled = pltpu.roll(quarter[j], shift, 1) if shift else quarter[j]
                laid = jnp.where((lane >= start) & (lane < start + 160), rolled, laid)
        slab[part] = laid.astype(BF16)
    for dy in range(1, 4):
        oy = mod(y + dy, 4)
        go(("m", dy), slab.at[oy], mid.at[y], y=oy)
    mid[y] = slab[y]

    arrived(("w", "w", 1), mw.at[east, ozl])
    go(("w", "w", 2), mw.at[east, ozl], mw.at[east, ozl], x=west)
    for dy in range(1, 4):
        arrived(("m", dy), mid.at[mod(y + 4 - dy, 4)])

    mine = zh * 2 + c
    head, tail = pl.ds(0, 2), pl.ds(2, 2)
    go("t0", mid.at[head], tok.at[mine, head], zh=right)
    go("t1", mid.at[tail], tok.at[mine, tail], zh=left)
    go("t2", mid, tok.at[mine], c=oc)
    go("t9", mid.at[tail], tok.at[mine, tail], zh=right)
    go("t10", mid.at[head], tok.at[mine, head], zh=left)
    tok[mine] = mid[...]
    load_q.wait()
    near_part()
    arrived(("k1", "u", 2), kw1.at[x, across, 0])
    arrived(("k1", "d", 2), kw1.at[x, across, 1])
    piece(across, 3)

    def piece_on(k, row):
        if k < 2:
            block, way, target = kw1.at[west, row], "e", east
        else:
            block, way, target = kw1.at[east, row], "w", west
        arrived(("k1", way, k), block)
        go(("k1", way, k, 2), block, block, x=target)

    arrived(("k0", "u"), kw0.at[down])
    go(("k0", "u", 2), kw0.at[down, pl.ds(0, 2)], kw0.at[down, pl.ds(0, 2)], y=up)
    arrived(("k0", "d"), kw0.at[up])
    go(("k0", "d", 2), kw0.at[up, pl.ds(2, 2)], kw0.at[up, pl.ds(2, 2)], y=down)
    piece_on(0, y)
    piece_on(1, down)
    piece_on(2, up)
    here, there = tok.at[left * 2 + c], tok.at[right * 2 + c]
    arrived("t0", here.at[head])
    go("t3", here.at[head], here.at[head], zh=right)
    arrived("t1", there.at[tail])
    go("t5", there.at[tail], there.at[tail], zh=left)
    arrived("t9", here.at[tail])
    go("t4", here, here, c=oc)
    arrived("t10", there.at[head])
    go("t6", there, there, c=oc)
    first, second = (tok.at[far * 2 + c].at[pl.ds(i, 2)] for i in (0, 2))
    arrived("t3", first)
    go("t7", first, first, c=oc)
    arrived("t5", second)
    go("t8", second, second, c=oc)
    arrived("t2", tok.at[zh * 2 + oc])
    arrived("t4", tok.at[left * 2 + oc])
    arrived("t6", tok.at[right * 2 + oc])
    arrived("t7", tok.at[far * 2 + oc].at[pl.ds(0, 2)])
    arrived("t8", tok.at[far * 2 + oc].at[pl.ds(2, 2)])
    arrived(("w", "w", 0), mw.at[east, zl])
    arrived(("w", "e", 1), mw.at[west, ozl])
    arrived(("w", "e", 2), mw.at[xfar, zl])
    arrived(("w", "w", 2), mw.at[xfar, ozl])

    def part(index):
        rows = tok[pl.ds(index * 2, 2)].reshape(128, VIT_D)
        return jnp.dot(rows, mw[...].reshape(VIT_D, 1024), preferred_element_type=F32)

    sb[0] = part(across).astype(BF16)
    go("s0", sb.at[0, pl.ds(0, 64)], ra.at[0], y=up)
    go("s1", sb.at[0, pl.ds(64, 64)], ra.at[1], y=down)
    nxt, prv = part(up), part(down)
    sb[1, 64:128] = nxt[64:128].astype(BF16)
    sb[2, 0:64] = prv[0:64].astype(BF16)
    go("s2", sb.at[1, pl.ds(64, 64)], rb.at[0, pl.ds(64, 64)], y=up)
    go("s3", sb.at[2, pl.ds(0, 64)], rb.at[1, pl.ds(0, 64)], y=down)
    piece_on(3, across)
    arrived("s0", ra.at[0])
    sb[1, 0:64] = (nxt[0:64] + ra[0].astype(F32)).astype(BF16)
    go("s4", sb.at[1, pl.ds(0, 64)], rb.at[0, pl.ds(0, 64)], y=up)
    arrived("s1", ra.at[1])
    sb[2, 64:128] = (prv[64:128] + ra[1].astype(F32)).astype(BF16)
    go("s5", sb.at[2, pl.ds(64, 64)], rb.at[1, pl.ds(64, 64)], y=down)
    own = part(y)
    arrived("s2", rb.at[0, pl.ds(64, 64)])
    arrived("s3", rb.at[1, pl.ds(0, 64)])
    arrived("s4", rb.at[0, pl.ds(0, 64)])
    arrived("s5", rb.at[1, pl.ds(64, 64)])
    embedded = (own + rb[0].astype(F32) + rb[1].astype(F32)).astype(BF16).astype(F32)
    square = jnp.sum(embedded * embedded, axis=1, keepdims=True)
    turned = jnp.transpose(jnp.broadcast_to(square, (128, 128)))
    others = [(dzh, dc) for dzh in range(4) for dc in range(2) if dzh or dc]
    ssr[zh * 2 + c] = turned[0:8]
    for dzh, dc in others:
        slot = ssr.at[zh * 2 + c]
        go(("q", dzh, dc), slot, slot, zh=mod(zh + dzh, 4), c=mod(c + dc, 2))
    scaled = (embedded * lm_gain[...][None, :]).astype(BF16)
    arrived(("k0", "u", 2), kw0.at[across, pl.ds(0, 2)])
    arrived(("k0", "d", 2), kw0.at[across, pl.ds(2, 2)])
    for k, row in enumerate((y, down, up, across)):
        if k < 2:
            arrived(("k1", "w", k), kw1.at[east, row])
            arrived(("k1", "e", k, 2), kw1.at[xfar, row])
        else:
            arrived(("k1", "e", k), kw1.at[west, row])
            arrived(("k1", "w", k, 2), kw1.at[xfar, row])

    def head_rows(k, t):
        kx, kz = 2 * k + t // 4, t % 4 // 2
        pieces = []
        for e in range(2):
            ky = 2 * (t % 2) + e
            pieces += [kw0[ky, kx, kz], kw1[kx, ky, kz]]
        return pieces

    for k in range(2):
        for t in range(0, 8, 2):
            both = jnp.concatenate(head_rows(k, t) + head_rows(k, t + 1), axis=0)
            both = nt_dot(scaled, both)
            kvf[k * 8 + t] = both[:, :128]
            kvf[k * 8 + t + 1] = both[:, 128:]

    for j in range(4):
        for k in range(2):
            cs[j, k] = kvf[k * 8 + j * 2 + oc].astype(BF16)
    go("c", cs, cr, c=oc)
    arrived("c", cr)

    def term(j, k):
        return kvf[k * 8 + j * 2 + c] + cr[j, k].astype(F32)

    for k in range(2):
        ks[0, k] = term(far, k).astype(BF16)
    go("z0", ks.at[0, 0], ka.at[0], zh=right)
    go("z1", ks.at[0, 1], ka.at[1], zh=left)
    ks[1, 1] = term(right, 1).astype(BF16)
    ks[2, 0] = term(left, 0).astype(BF16)
    go("z2", ks.at[1, 1], kb.at[0, 1], zh=right)
    go("z3", ks.at[2, 0], kb.at[1, 0], zh=left)
    arrived("z0", ka.at[0])
    ks[1, 0] = (term(right, 0) + ka[0].astype(F32)).astype(BF16)
    go("z4", ks.at[1, 0], kb.at[0, 0], zh=right)
    arrived("z1", ka.at[1])
    ks[2, 1] = (term(left, 1) + ka[1].astype(F32)).astype(BF16)
    go("z5", ks.at[2, 1], kb.at[1, 1], zh=left)
    for dzh, dc in others:
        arrived(("q", dzh, dc), ssr.at[mod(zh + 4 - dzh, 4) * 2 + mod(c + dc, 2)])
    total = jnp.sum(ssr[...], axis=0)[0:1]
    factor = lax.rsqrt(jnp.broadcast_to(total, (128, 128)) / D + 1e-6)
    factor = jnp.transpose(factor)
    arrived("z2", kb.at[0, 1])
    arrived("z3", kb.at[1, 0])
    arrived("z4", kb.at[0, 0])
    arrived("z5", kb.at[1, 1])
    for k in range(2):
        done = term(zh, k) + kb[0, k].astype(F32) + kb[1, k].astype(F32)
        vis[y, zl, k] = (done * factor).astype(BF16)

    first = vis.at[y, zl]
    go("v0", first, first, zl=ozl)
    go("v1", first, first, y=up)
    go("v2", first, first, y=down)
    second = vis.at[y, ozl]
    arrived("v0", second)
    go("v3", second, second, y=up)
    go("v4", second, second, y=down)
    below = vis.at[down, zl]
    arrived("v1", below)
    go("v5", below, below, y=up)
    arrived("v2", vis.at[up, zl])

    def keep(i, total, top):
        lacc[lm_rows(i), :] = total
        lpeak[lm_rows(i), :] = top

    def pass_up(i):
        if i == 3:
            above = vis.at[up, ozl]
            arrived("v4", above)
            go("v6", above, above, y=down)

    far_part([(y, zl), (y, ozl), (down, zl), (up, zl)], keep, pass_up)
    arrived("v3", vis.at[down, ozl])
    arrived("v5", vis.at[across, zl])
    arrived("v6", vis.at[across, ozl])
    stores = []

    def finish(i, total, top):
        result[lm_rows(i), :] = (total[:, :HD] / total[:, HD:]).astype(BF16)

    def write(i):
        if i % 4 == 3:
            rows = pl.ds((i - 3) * 256, 1024)
            copy = pltpu.make_async_copy(result.at[rows], out.at[rows], w_sem.at[17 + i // 4])
            copy.start()
            stores.append(copy)

    far_part([(down, ozl), (up, ozl), (across, zl), (across, ozl)], finish, write)
    assert len(numbers) == COPIES, len(numbers)
    for copy in sends:
        copy.wait_send()
    for copy in stores:
        copy.wait()


def attend(counts, qkv, wo, gain, merger, kvw, lm_gain, queries, span):
    dma = pltpu.SemaphoreType.DMA
    vmem = pl.BlockSpec(memory_space=pltpu.VMEM)
    hbm = pl.BlockSpec(memory_space=pl.ANY)
    return pl.pallas_call(
        front_kernel,
        out_shape=jax.ShapeDtypeStruct(queries.shape, BF16),
        in_specs=[
            pl.BlockSpec(memory_space=pltpu.SMEM), vmem, hbm, vmem, vmem, vmem, vmem, hbm, vmem,
        ],
        out_specs=hbm,
        scratch_shapes=[
            pltpu.VMEM((16, 64, PACKED), BF16),
            pltpu.VMEM((4, 16, 64, PACKED), BF16),
            pltpu.VMEM((1024, PACKED), BF16),
            pltpu.VMEM((1024, PACKED), F32),
            pltpu.VMEM((1024, HD), F32),
            pltpu.VMEM((16, 64, HD), BF16),
            pltpu.VMEM((16, 64, HD), BF16),
            pltpu.VMEM((16, HD, VIT_D), BF16),
            pltpu.VMEM((64 * VIT_D // HD, HD), F32),
            pltpu.VMEM((4, 16, VIT_D), BF16),
            pltpu.VMEM((4, 16, VIT_D), BF16),
            pltpu.VMEM((8, 4, 16, VIT_D), BF16),
            pltpu.VMEM((4, 2, 160, 1024), BF16),
            pltpu.VMEM((4, 4, 2, LOW, 1024), BF16),
            pltpu.VMEM((4, 4, 2, 64 - LOW, 1024), BF16),
            pltpu.VMEM((3, 128, 1024), BF16),
            pltpu.VMEM((2, 64, 1024), BF16),
            pltpu.VMEM((2, 128, 1024), BF16),
            pltpu.VMEM((16, 128, 128), F32),
            pltpu.VMEM((4, 2, 128, 128), BF16),
            pltpu.VMEM((4, 2, 128, 128), BF16),
            pltpu.VMEM((3, 2, 128, 128), BF16),
            pltpu.VMEM((2, 128, 128), BF16),
            pltpu.VMEM((2, 2, 128, 128), BF16),
            pltpu.VMEM((8, 8, 128), F32),
            pltpu.VMEM((4, 2, 2, 128, 128), BF16),
            pltpu.VMEM((4096, HD), BF16),
            pltpu.VMEM((4096, 2 * HD), F32),
            pltpu.VMEM((4096, HD), F32),
            pltpu.VMEM((4096, HD), BF16),
            dma((21,)), dma((COPIES,)), dma((COPIES,)),
        ],
        compiler_params=pltpu.CompilerParams(
            collective_id=0, has_side_effects=True, vmem_limit_bytes=61 * 2**20
        ),
        cost_estimate=pl.CostEstimate(
            flops=60_000_000_000, bytes_accessed=8_000_000, transcendentals=4_200_000
        ),
        name="front",
    )(counts, qkv, wo, gain, merger, kvw, lm_gain, queries, span)


def local(
    vit_qkv,
    patch_counts,
    vit_out_weight,
    vit_norm_gain,
    merger_weight,
    lm_norm_gain,
    kv_weight,
    queries,
    span_kv,
):
    rows = queries.shape[1] * queries.shape[2]
    span = span_kv[0, :, :, 0].transpose(1, 0, 2)
    out = attend(
        patch_counts, vit_qkv[0].transpose(1, 0, 2), vit_out_weight, vit_norm_gain,
        merger_weight, kv_weight.T, lm_norm_gain, queries.reshape(rows, HD), span,
    )
    return out.reshape(queries.shape)


def solution(mesh):
    fine = Mesh(mesh.devices.reshape(4, 2, 4, 4, 2), ("x", "zl", "y", "zh", "c"))
    placed = (
        P("x", (*SEQ, *TP), None, None),
        P("x"),
        P(),
        P(),
        P(IMG_SEQ, TP),
        P(TP),
        P(TP, IMG_SEQ),
        P("x", SEQ, TP, None),
        P("x", SEQ, None, TP, None),
    )
    return jax.shard_map(
        local, mesh=fine, in_specs=placed, out_specs=P("x", SEQ, TP, None), check_vma=False
    )
```
